128 devices in a mesh: rep: 1, r: 4 (over x), s: 32 (over y, z, core).
Axes of the slice: x: 4, y: 4, z: 4, core: 2. Of those that a mesh axis runs over, the one named last changes fastest.
Arguments:
- x: bfloat16 [128, 2048, 1280], P(('rep', 'r', 's'))
- dy: bfloat16 [128, 2048, 1280], P(('rep', 'r', 's'))
- w_gate: bfloat16 [2, 1280, 4864], P(None, 's')
- w_up: bfloat16 [2, 1280, 4864], P(None, 's')
- w_down: bfloat16 [2, 4864, 1280], P(None, 's')
- m_w_gate: float32 [2, 1280, 4864], P(None, 's')
- m_w_up: float32 [2, 1280, 4864], P(None, 's')
- m_w_down: float32 [2, 4864, 1280], P(None, 's')
- v_w_gate: float32 [2, 1280, 4864], P(None, 's')
- v_w_up: float32 [2, 1280, 4864], P(None, 's')
- v_w_down: float32 [2, 4864, 1280], P(None, 's')
Outputs:
- output 1: bfloat16 [2, 1280, 4864], P('rep', 's')
- output 2: bfloat16 [2, 1280, 4864], P('rep', 's')
- output 3: bfloat16 [2, 4864, 1280], P('rep', 's')
- output 4: float32 [2, 1280, 4864], P('rep', 's')
- output 5: float32 [2, 1280, 4864], P('rep', 's')
- output 6: float32 [2, 4864, 1280], P('rep', 's')
- output 7: float32 [2, 1280, 4864], P('rep', 's')
- output 8: float32 [2, 1280, 4864], P('rep', 's')
- output 9: float32 [2, 4864, 1280], P('rep', 's')
All inputs are finite; a program needn't handle non-finite values.
Results may differ from the reference program's by a relative error of at most 0.022.
Values are sent between devices in bfloat16 or wider.
A program may use at most 1.5 GiB of HBM per device.

```python
import jax
import jax.numpy as jnp
from jax import lax

SEQUENCES = 128
TOKENS = 2048
D = 1280
FF = 4864
LAYERS = 2
NAMES = ("w_gate", "w_up", "w_down")
SHAPES = {"w_gate": (LAYERS, D, FF), "w_up": (LAYERS, D, FF), "w_down": (LAYERS, FF, D)}


def bump(key, n, height):
    away = (jnp.arange(n, dtype=jnp.int32) - jax.random.randint(key, (), 0, n, jnp.int32)) % n
    return jnp.where(away < n // 8, height, 1.0)


def together(key, own, strength):
    shared = jax.random.normal(key, own.shape[1:], jnp.float32)
    return (own + strength * shared) * lax.rsqrt(1 + strength * strength)


def setup_inputs(seed: int = 0, part: int = 0) -> dict:
    kx, kdy, ka, kb, kz, kf, kh, kl, *keys = jax.random.split(jax.random.key(seed), 8 + 3 * len(NAMES))
    kx, kdy, ka, kb = (jax.random.fold_in(k, part) for k in (kx, kdy, ka, kb))
    kw, km, kv = (keys[i::3] for i in range(3))
    shape = (SEQUENCES, TOKENS, D)
    much_x, much_dy = jax.random.uniform(kz, (2,), jnp.float32, 0.0, 1.0)
    loud = 2.0 ** jax.random.uniform(jax.random.fold_in(kz, 1), (), jnp.float32, -1.0, 2.0)
    layers = 2.0 ** jax.random.uniform(kl, (LAYERS, 1, 1), jnp.float32, -1.0, 1.0)
    x = together(ka, jax.random.normal(kx, shape, jnp.float32), much_x) * bump(kf, D, 4.0)
    dy = together(kb, jax.random.normal(kdy, shape, jnp.float32), much_dy)
    drawn = {"x": x.astype(jnp.bfloat16), "dy": (loud * dy * (SEQUENCES * TOKENS) ** -0.5).astype(jnp.bfloat16)}
    for key, name in zip(kw, NAMES, strict=True):
        w = jax.random.normal(key, SHAPES[name], jnp.float32) * SHAPES[name][1] ** -0.5
        drawn[name] = (w * {"w_gate": 1.0, "w_up": bump(kh, FF, 4.0), "w_down": layers}[name]).astype(jnp.bfloat16)
    for key, name in zip(km, NAMES, strict=True):
        drawn[f"m_{name}"] = 0.1 * jax.random.normal(key, SHAPES[name], jnp.float32)
    for key, name in zip(kv, NAMES, strict=True):
        drawn[f"v_{name}"] = jax.random.uniform(key, SHAPES[name], jnp.float32, 0.005, 0.015)
    return drawn


def matmul(a, w):
    return jnp.dot(a, w, preferred_element_type=jnp.float32).astype(jnp.bfloat16)


def normed(h):
    wide = h.astype(jnp.float32)
    scale = lax.rsqrt(jnp.mean(wide**2, -1, keepdims=True) + 1e-6)
    return (wide * scale).astype(jnp.bfloat16)


def layer(h, w):
    a = normed(h)
    gate = jnp.dot(a, w["w_gate"], preferred_element_type=jnp.float32)
    up = jnp.dot(a, w["w_up"], preferred_element_type=jnp.float32)
    return h + matmul((jax.nn.silu(gate) * up).astype(jnp.bfloat16), w["w_down"])


def adamw(w, m, v, g):
    m = 0.9 * m + 0.1 * g
    v = 0.95 * v + 0.05 * g * g
    step = m * lax.rsqrt(v + 1e-8) + 0.1 * w
    return (w - 0.02 * step).astype(jnp.bfloat16), m, v


def clipped(gradients, sum_of_squares, count):
    factor = jnp.minimum(1.0, 0.5 * lax.rsqrt(sum_of_squares / count + 1e-30))
    return [g * factor for g in gradients]


def stack(weights, h):
    return lax.scan(lambda h, w: (layer(h, w), None), h, weights)[0]


def reference(x, dy, w_gate, w_up, w_down, m_w_gate, m_w_up, m_w_down, v_w_gate, v_w_up, v_w_down):
    weights = dict(zip(NAMES, (w_gate, w_up, w_down), strict=True))

    def take(so_far, sequence):
        h, by_y = sequence
        _, back = jax.vjp(lambda w: stack(w, h), weights)
        return jax.tree.map(lambda total, term: total + term.astype(jnp.float32), so_far, back(by_y)[0]), None

    none_yet = {name: jnp.zeros(w.shape, jnp.float32) for name, w in weights.items()}
    by_weights, _ = lax.scan(take, none_yet, (x, dy))
    gradients = [by_weights[name].astype(jnp.bfloat16).astype(jnp.float32) for name in NAMES]
    gradients = clipped(gradients, sum(jnp.sum(g * g) for g in gradients), sum(g.size for g in gradients))
    new = [
        adamw(w.astype(jnp.float32), m, v, g)
        for w, m, v, g in zip((w_gate, w_up, w_down), (m_w_gate, m_w_up, m_w_down), (v_w_gate, v_w_up, v_w_down), gradients, strict=True)
    ]
    return tuple(one[which] for which in range(3) for one in new)
```

```python
import functools

import jax
import jax.numpy as jnp
from jax import lax
from jax.experimental import pallas as pl
from jax.experimental.pallas import tpu as pltpu
from jax.sharding import PartitionSpec as P

NAMES = ("w_gate", "w_up", "w_down")
BF, F32 = jnp.bfloat16, jnp.float32
MESH = pl.DeviceIdType.MESH

TOKENS, D, FF = 2048, 1280, 4864
NY = NZ = NX = 4
S = NY * NZ * 2
RD, RF = D // S, FF // S
TF = 256
NT = FF // TF
ND = D // TF
VMEM_LIMIT = 67_000_000


def dot(a, b, ca, cb):
    return lax.dot_general(a, b, (((ca,), (cb,)), ((), ())), preferred_element_type=F32)


def at(*index):
    return index


def above(i):
    return i * ((i + 64) // 64)


def upto(i, last):
    return last - above(last - i)


def cols(start, size):
    return pl.ds(pl.multiple_of(start, 128), size)


class Place:
    def __init__(self):
        s = lax.axis_index("s")
        self.y, self.z, self.c = lax.div(s, NZ * 2), lax.rem(lax.div(s, 2), NZ), lax.rem(s, 2)
        self.x = lax.axis_index("r")
        self.pos = (self.y, self.z)

    def ring(self, axis, by):
        return lax.rem(self.pos[axis] + by, 4)

    def near(self, axis, by):
        y, z = (self.ring(0, by), self.z) if axis == 0 else (self.y, self.ring(1, by))
        return {"s": (y * NZ + z) * 2 + self.c}

    def partner(self):
        return {"s": (self.y * NZ + self.z) * 2 + 1 - self.c}

    def across(self, by):
        return {"r": lax.rem(self.x + by, NX)}

    def meet(self, x_too):
        barrier = pltpu.get_barrier_semaphore()
        peers = [self.near(axis, by) for axis in (0, 1) for by in (1, 3)] + [self.partner()]
        if x_too:
            peers += [self.across(by) for by in (1, 2, 3)]
        for peer in peers:
            pl.semaphore_signal(barrier, inc=1, device_id=peer, device_id_type=MESH)
        pl.semaphore_wait(barrier, len(peers))


def wait_bytes(ref, sem):
    pltpu.make_async_copy(ref, ref, sem).wait()


CH = NT + ND
LAG = 2
LEAD = 5 * LAG + 1


def gather_kernel(a, wgu, wd, g_gu, g_d, act, gate, up, wt, ssem, rsem, lsem, osem):
    step = pl.program_id(0)
    i = step - LEAD
    me = Place()
    own = [
        pltpu.make_async_copy(wgu, g_gu.at[:, me.y, me.z, me.c], osem.at[0]),
        pltpu.make_async_copy(wd, g_d.at[me.y, me.z, me.c], osem.at[1]),
    ]

    @pl.when(step == 0)
    def _():
        me.meet(False)
        for copy in own:
            copy.start()

    @pl.when(step == 2 * LAG)
    def _():
        for copy in own:
            copy.wait()

    def block(kind, t, half, sub, y, z, c):
        width = TF if half is None else TF // 2
        start = t * TF + (half or 0) * (TF // 2)
        if kind == "gu":
            lead = slice(None) if sub is None else sub
            return g_gu.at[lead, y, z, c, :, cols(start, width)]
        rows = {None: slice(None), 0: pl.ds(0, 80), 1: pl.ds(80, RF - 80)}[sub]
        return g_d.at[y, z, c, rows, cols(start, width)]

    def mine(kind, t, half):
        start = t * TF + half * (TF // 2)
        return wgu.at[:, :, cols(start, TF // 2)] if kind == "gu" else wd.at[:, cols(start, TF // 2)]

    ALL = slice(None)

    def totals(kind, t, k):
        c = me.c
        y, z = [(pl.ds(0, 2), 0), (pl.ds(0, 1), 0), (ALL, pl.ds(0, 2)), (ALL, pl.ds(0, 1)), (ALL, ALL)][k]
        return block(kind, t, None, None, y, z, c)

    def send(kind, t, ch, k):
        def go(src, dst, peer):
            pltpu.make_async_remote_copy(
                src_ref=src, dst_ref=dst, send_sem=ssem.at[k, ch], recv_sem=rsem.at[k, ch], device_id=peer, device_id_type=MESH
            ).start()

        y, z, c = me.y, me.z, me.c
        for half in (0, 1):
            first, second = (0, 1) if half == 0 else (1, 0)
            if k == 0:
                for by in (1, 3):
                    go(mine(kind, t, half), block(kind, t, half, None, y, z, c), me.near(first, by))
            if k == 1:
                for sub, by in ((0, 1), (1, 3)):
                    back = me.ring(first, 4 - by)
                    ref = block(kind, t, half, sub, *((back, z) if first == 0 else (y, back)), c)
                    go(ref, ref, me.near(first, by))
            if k == 2:
                ref = block(kind, t, half, None, *((ALL, z) if first == 0 else (y, ALL)), c)
                for by in (1, 3):
                    go(ref, ref, me.near(second, by))
            if k == 3:
                for sub, by in ((0, 1), (1, 3)):
                    back = me.ring(second, 4 - by)
                    ref = block(kind, t, half, sub, *((ALL, back) if second == 1 else (back, ALL)), c)
                    go(ref, ref, me.near(second, by))
        if k == 4:
            ref = block(kind, t, None, None, ALL, ALL, c)
            go(ref, ref, me.partner())

    def load(t):
        return pltpu.make_async_copy(g_gu.at[:, :, :, :, :, cols(t * TF, TF)], wt.at[lax.rem(t, 2)], lsem.at[lax.rem(t, 2)])

    for k in (5, 4, 3, 2, 1, 0):
        ch = i + 1 + (5 - k) * LAG
        for kind, low, high in (("gu", 0, NT), ("d", NT, CH)):

            @pl.when((ch >= low) & (ch < high))
            def _(k=k, kind=kind, t=ch - low, ch=ch):
                if k > 0:
                    wait_bytes(totals(kind, t, k - 1), rsem.at[k - 1, ch])
                if k < 5:
                    send(kind, t, ch, k)
                elif kind == "gu":
                    load(t).start()

    @pl.when((i >= 0) & (i < NT))
    def _():
        load(i).wait()
        slot = lax.rem(i, 2)
        rows = TOKENS // 4
        for r in range(4):
            part = pl.ds(r * rows, rows)
            g = dot(a[part, :], wt[slot, 0].reshape(D, TF), 1, 0)
            u = dot(a[part, :], wt[slot, 1].reshape(D, TF), 1, 0)
            gate[part, :] = g
            up[part, :] = u
            act[part, :] = (g * jax.nn.sigmoid(g) * u).astype(BF)

    @pl.when(step == LEAD + CH - 2)
    def _():
        for k in range(5):
            for kind, low, high in (("gu", 0, NT), ("d", NT, CH)):

                @pl.loop(low, high)
                def _(ch, k=k, kind=kind, low=low):
                    wait_bytes(totals(kind, ch - low, k), ssem.at[k, ch])


def gathered(a, wgu, wd, number):
    tile = pl.BlockSpec((TOKENS, TF), lambda step: (0, upto(above(step - LEAD), NT - 1)))
    vmem, hbm = pl.BlockSpec(memory_space=pltpu.VMEM), pl.BlockSpec(memory_space=pl.ANY)
    g_gu, g_d, *rest = pl.pallas_call(
        gather_kernel,
        grid=(LEAD + CH - 1,),
        in_specs=[vmem, vmem, vmem],
        out_specs=[hbm, hbm, tile, tile, tile],
        out_shape=[
            jax.ShapeDtypeStruct((2, NY, NZ, 2, RD, FF), BF),
            jax.ShapeDtypeStruct((NY, NZ, 2, RF, D), BF),
            jax.ShapeDtypeStruct((TOKENS, FF), BF),
            jax.ShapeDtypeStruct((TOKENS, FF), F32),
            jax.ShapeDtypeStruct((TOKENS, FF), F32),
        ],
        scratch_shapes=[
            pltpu.VMEM((2, 2, NY, NZ, 2, RD, TF), BF),
            pltpu.SemaphoreType.DMA((5, CH)),
            pltpu.SemaphoreType.DMA((5, CH)),
            pltpu.SemaphoreType.DMA((2,)),
            pltpu.SemaphoreType.DMA((2,)),
        ],
        compiler_params=pltpu.CompilerParams(
            collective_id=number, has_side_effects=True, vmem_limit_bytes=VMEM_LIMIT, dimension_semantics=("arbitrary",)
        ),
        cost_estimate=pl.CostEstimate(flops=4 * TOKENS * D * FF, bytes_accessed=200_000_000, transcendentals=TOKENS * FF),
        name=f"gather_{number}",
    )(a, wgu, wd)
    return g_gu.reshape(2, D, FF), g_d.reshape(FF, D), *rest


DC = 128
NDC = D // DC
TAIL = 7


class Summing:
    HEIGHTS = {"gu": ((RD, RD), (RD, RD)), "d": ((40, 40), (40, RF - 120))}

    def __init__(self, kind, count, entry, me, own, inbox, s1, r2, s2, r3, acc, s4, r4, s5, r5, xb, ssem, rsem, out):
        self.kind, self.count, self.entry, self.me = kind, count, entry, me
        self.own, self.inbox, self.s1, self.r2, self.s2, self.r3 = own, inbox, s1, r2, s2, r3
        self.acc, self.s4, self.r4, self.s5, self.r5, self.xb = acc, s4, r4, s5, r5, xb
        self.ssem, self.rsem, self.out = ssem, rsem, out
        self.subs = (slice(None),) if kind == "gu" else (0, 1)

    def part(self, half, sub):
        if self.kind == "gu":
            return sub, slice(None), pl.ds(half * 128, 128)
        low = 80 * half + 40 * sub
        return 0, pl.ds(low, self.HEIGHTS["d"][half][sub]), slice(None)

    def rows(self, half, sub):
        return slice(None) if self.kind == "gu" else pl.ds(0, self.HEIGHTS["d"][half][sub])

    def both(self, slot, y, z, half, sub):
        lead, rows, columns = self.part(half, sub)
        mine = self.own[slot, lead, y, z, self.me.c, rows, columns] if self.kind == "gu" else self.own[slot, y, z, rows, columns]
        theirs = self.inbox[slot, lead, y, z, rows, columns] if self.kind == "gu" else self.inbox[slot, y, z, rows, columns]
        return mine.astype(F32) + theirs.astype(F32)

    def size(self, k, slot, two):
        if k == 0:
            return self.inbox.at[slot]
        if k == 5:
            return self.xb.at[two, pl.ds(0, 3)]
        if self.kind == "gu":
            return (self.r2, self.r3, self.r4, self.r5)[k - 1].at[two]
        return self.inbox.at[(slot, *((0,), (pl.ds(0, 2),), (0, 0), (0, pl.ds(0, 2)))[k - 1])]

    def compute(self, k, t):
        me, slot, two = self.me, lax.rem(t, 4), lax.rem(t, 2)
        if k > 0:
            wait_bytes(self.size(k - 1, slot, two), self.rsem.at[k - 1, slot])
            wait_bytes(self.size(k - 1, slot, two), self.ssem.at[k - 1, slot])
        if k == 6:
            total = self.xb[two, 0].astype(F32)
            for x in range(1, NX):
                total = total + self.xb[two, x].astype(F32)
            if self.kind == "gu":
                self.out[:, :, cols(t * TF, TF)] = total.astype(BF)
            else:
                self.out[:, cols(t * DC, DC)] = total.astype(BF)
            return
        for half in (0, 1):
            first, second = (0, 1) if half == 0 else (1, 0)
            along = lambda place: (place, slice(None)) if first == 0 else (slice(None), place)
            for sub in (0, 1):
                rows = self.rows(half, sub)
                if k == 1:
                    self.s1[half, sub, :, rows] = self.both(slot, *along(me.ring(first, 2)), half, sub).astype(BF)
                if k == 2:
                    for way, by in ((0, 1), (1, 3)):
                        term = self.both(slot, *along(me.ring(first, by)), half, sub)
                        if sub == way:
                            term = term + self.r2[two, half, sub, :, rows].astype(F32)
                        self.s2[half, way, sub, :, rows] = term.astype(BF)
                if k == 3:
                    term = self.both(slot, *along(me.pos[first]), half, sub)
                    for way in (0, 1):
                        term = term + self.r3[two, half, way, sub, :, rows].astype(F32)
                    self.acc[two, half, sub, :, rows] = term
                    self.s4[half, sub, rows] = self.acc[two, half, sub, me.ring(second, 2), rows].astype(BF)
                if k == 4:
                    for way, by in ((0, 1), (1, 3)):
                        term = self.acc[two, half, sub, me.ring(second, by), rows]
                        if sub == way:
                            term = term + self.r4[two, half, sub, rows].astype(F32)
                        self.s5[half, way, sub, rows] = term.astype(BF)
                if k == 5:
                    term = self.acc[two, half, sub, me.pos[second], rows]
                    for way in (0, 1):
                        term = term + self.r5[two, half, way, sub, rows].astype(F32)
                    lead, where, columns = self.part(half, sub)
                    if self.kind == "gu":
                        self.xb[two, me.x, lead, where, columns] = term.astype(BF)
                    else:
                        self.xb[two, me.x, where, columns] = term.astype(BF)

    def send(self, k, t, source=None):
        me, slot, two = self.me, lax.rem(t, 4), lax.rem(t, 2)

        def go(src, dst, peer):
            pltpu.make_async_remote_copy(
                src_ref=src, dst_ref=dst, send_sem=self.ssem.at[k, slot], recv_sem=self.rsem.at[k, slot], device_id=peer, device_id_type=MESH
            ).start()

        if k == 0:
            go(source, self.inbox.at[slot], me.partner())
        if k == 5:
            for by in (1, 2, 3):
                go(self.xb.at[two, me.x], self.xb.at[two, me.x], me.across(by))
        for half in (0, 1):
            first, second = (0, 1) if half == 0 else (1, 0)
            for way, by in ((0, 1), (1, 3)):
                if k == 1:
                    rows = self.rows(half, way)
                    go(self.s1.at[half, way, :, rows], self.r2.at[two, half, way, :, rows], me.near(first, by))
                if k == 3:
                    rows = self.rows(half, way)
                    go(self.s4.at[half, way, rows], self.r4.at[two, half, way, rows], me.near(second, by))
                if k in (2, 4):
                    for sub in self.subs:
                        rows = self.rows(half, sub)
                        if k == 2:
                            go(self.s2.at[half, way, sub, :, rows], self.r3.at[two, half, way, sub, :, rows], me.near(first, by))
                        else:
                            go(self.s5.at[half, way, sub, rows], self.r5.at[two, half, way, sub, rows], me.near(second, by))


def stage_buffers(kind):
    block = (2, NY, NZ, RD, TF) if kind == "gu" else (NY, NZ, RF, DC)
    last = (2, RD, TF) if kind == "gu" else (RF, DC)
    return [
        pltpu.VMEM((4, 2, NY, NZ, 2, RD, TF) if kind == "gu" else (4, *block), BF),
        pltpu.VMEM((4, *block), BF),
        pltpu.VMEM((2, 2, 4, 40, 128), BF),
        pltpu.VMEM((2, 2, 2, 4, 40, 128), BF),
        pltpu.VMEM((2, 2, 2, 4, 40, 128), BF),
        pltpu.VMEM((2, 2, 2, 2, 4, 40, 128), BF),
        pltpu.VMEM((2, 2, 2, 4, 40, 128), F32),
        pltpu.VMEM((2, 2, 40, 128), BF),
        pltpu.VMEM((2, 2, 2, 40, 128), BF),
        pltpu.VMEM((2, 2, 2, 40, 128), BF),
        pltpu.VMEM((2, 2, 2, 2, 40, 128), BF),
        pltpu.VMEM((2, NX, *last), BF),
        pltpu.SemaphoreType.DMA((6, 4)),
        pltpu.SemaphoreType.DMA((6, 4)),
    ]


NBUF = 14


def back_kernel(with_da, *refs):
    refs = list(refs)
    take = lambda n: [refs.pop(0) for _ in range(n)]
    a, dy, wd, gate, up, dwd = take(6)
    wgu = take(1)[0] if with_da else None
    out_gu, out_d = take(2)
    da = take(1)[0] if with_da else None
    gu_bufs, d_bufs = take(NBUF), take(NBUF)
    dg_s, du_s, lsem = take(3)
    i = pl.program_id(0)
    me = Place()

    @pl.when(i == 0)
    def _():
        me.meet(True)

    own = gu_bufs[0]
    gu = Summing("gu", NT, 1, me, *gu_bufs, out_gu)
    down = Summing("d", NDC, 1, me, *d_bufs, out_d)

    def load(n):
        return pltpu.make_async_copy(dwd.at[:, :, me.c, :, cols(n * DC, DC)], down.own.at[lax.rem(n, 4)], lsem.at[lax.rem(n, 4)])

    for k in (6, 5, 4, 3, 2, 1):
        for engine in (gu, down):
            t = i - engine.entry - k

            @pl.when((t >= 0) & (t < engine.count))
            def _(k=k, engine=engine, t=t):
                if k == 1 and engine is down:
                    load(t).wait()
                engine.compute(k, t)

    for k in (5, 4, 3, 2, 1, 0):
        for engine in (gu, down):
            t = i - engine.entry - k

            @pl.when((t >= 0) & (t < engine.count))
            def _(k=k, engine=engine, t=t):
                source = None
                if k == 0:
                    source = own.at[lax.rem(t, 4), :, :, :, 1 - me.c] if engine is gu else dwd.at[:, :, 1 - me.c, :, cols(t * DC, DC)]
                engine.send(k, t, source)

    @pl.when(i < NDC)
    def _():
        load(i).start()

    @pl.when(i < NT)
    def _():
        slot = lax.rem(i, 4)
        rows = TOKENS // 4
        for r in range(4):
            part = pl.ds(r * rows, rows)
            dh = dot(dy[part, :], wd[...], 1, 1).astype(BF).astype(F32)
            g, u = gate[part, :], up[part, :]
            sg = jax.nn.sigmoid(g)
            du_s[part, :] = (dh * (g * sg)).astype(BF)
            dg_s[part, :] = (dh * u * (sg * (1 + g * (1 - sg)))).astype(BF)
        own[slot, 0] = dot(a[...], dg_s[...], 0, 0).reshape(NY, NZ, 2, RD, TF).astype(BF)
        own[slot, 1] = dot(a[...], du_s[...], 0, 0).reshape(NY, NZ, 2, RD, TF).astype(BF)
        if with_da:
            for r in range(4):
                part = pl.ds(r * rows, rows)
                more = dot(dg_s[part, :], wgu[0], 1, 1) + dot(du_s[part, :], wgu[1], 1, 1)

                @pl.when(i == 0)
                def _():
                    da[part, :] = more

                @pl.when(i > 0)
                def _():
                    da[part, :] += more


def backward(a, dy, g_d, gate, up, dwd, g_gu, number):
    with_da = g_gu is not None
    last = lambda i: upto(i, NT - 1)
    vmem, hbm = pl.BlockSpec(memory_space=pltpu.VMEM), pl.BlockSpec(memory_space=pl.ANY)
    tile = pl.BlockSpec((TOKENS, TF), lambda i: (0, last(i)))
    in_specs = [vmem, vmem, pl.BlockSpec((TF, D), lambda i: (last(i), 0)), tile, tile, hbm]
    out_shape = [jax.ShapeDtypeStruct((2, RD, FF), BF), jax.ShapeDtypeStruct((RF, D), BF)]
    operands = [a, dy, g_d, gate, up, dwd.reshape(NY, NZ, 2, RF, D)]
    if with_da:
        in_specs.append(pl.BlockSpec((2, D, TF), lambda i: (0, 0, last(i))))
        out_shape.append(jax.ShapeDtypeStruct((TOKENS, D), F32))
        operands.append(g_gu)
    return pl.pallas_call(
        functools.partial(back_kernel, with_da),
        grid=(NT + TAIL,),
        in_specs=in_specs,
        out_specs=[vmem] * len(out_shape),
        out_shape=out_shape,
        scratch_shapes=[
            *stage_buffers("gu"),
            *stage_buffers("d"),
            pltpu.VMEM((TOKENS, TF), BF),
            pltpu.VMEM((TOKENS, TF), BF),
            pltpu.SemaphoreType.DMA((4,)),
        ],
        compiler_params=pltpu.CompilerParams(
            collective_id=number, has_side_effects=True, vmem_limit_bytes=VMEM_LIMIT, dimension_semantics=("arbitrary",)
        ),
        cost_estimate=pl.CostEstimate(
            flops=(10 if with_da else 6) * TOKENS * D * FF, bytes_accessed=200_000_000, transcendentals=TOKENS * FF
        ),
        name=f"backward_{number}",
    )(*operands)


def total_kernel(part, out, b0, b1, b2, ssem, rsem):
    me = Place()
    barrier = pltpu.get_barrier_semaphore()
    rings = [[me.near(axis, by) for by in (1, 2, 3)] for axis in (0, 1)] + [[me.partner()]]
    peers = [peer for ring in rings for peer in ring]
    for peer in peers:
        pl.semaphore_signal(barrier, inc=1, device_id=peer, device_id_type=MESH)
    pl.semaphore_wait(barrier, len(peers))
    value = part[...]
    for k, (buf, place, ring) in enumerate(zip((b0, b1, b2), (me.y, me.z, me.c), rings, strict=True)):
        buf[place] = value
        for peer in ring:
            pltpu.make_async_remote_copy(
                src_ref=buf.at[place], dst_ref=buf.at[place], send_sem=ssem.at[k], recv_sem=rsem.at[k], device_id=peer, device_id_type=MESH
            ).start()
        wait_bytes(buf.at[pl.ds(0, len(ring))], rsem.at[k])
        wait_bytes(buf.at[pl.ds(0, len(ring))], ssem.at[k])
        value = buf[0]
        for n in range(1, len(ring) + 1):
            value = value + buf[n]
    out[...] = value


def over_group(number, collective):
    part = jnp.full((8, 128), number, F32)
    vmem = pl.BlockSpec(memory_space=pltpu.VMEM)
    out = pl.pallas_call(
        total_kernel,
        in_specs=[vmem],
        out_specs=vmem,
        out_shape=jax.ShapeDtypeStruct((8, 128), F32),
        scratch_shapes=[
            pltpu.VMEM((NY, 8, 128), F32),
            pltpu.VMEM((NZ, 8, 128), F32),
            pltpu.VMEM((2, 8, 128), F32),
            pltpu.SemaphoreType.DMA((3,)),
            pltpu.SemaphoreType.DMA((3,)),
        ],
        compiler_params=pltpu.CompilerParams(collective_id=collective, has_side_effects=True),
        name="total",
    )(part)
    return out[0, 0]


def normed(h):
    wide = h.astype(F32)
    scale = lax.rsqrt(jnp.mean(wide**2, -1, keepdims=True) + 1e-6)
    return (wide * scale).astype(BF)


def adamw(w, m, v, g):
    m = 0.9 * m + 0.1 * g
    v = 0.95 * v + 0.05 * g * g
    step = m * lax.rsqrt(v + 1e-8) + 0.1 * w
    return (w - 0.02 * step).astype(BF), m, v


def clipped(gradients, sum_of_squares, count):
    factor = jnp.minimum(1.0, 0.5 * lax.rsqrt(sum_of_squares / count + 1e-30))
    return [g * factor for g in gradients]


def solution(mesh):
    def step(x, dy, *arrays):
        weights, m, v = (arrays[i : i + 3] for i in (0, 3, 6))
        shards = lambda layer: (jnp.stack([weights[0][layer], weights[1][layer]]), weights[2][layer])
        h0, dy = x[0], dy[0]
        a0 = normed(h0)
        gu0, d0, act0, gate0, up0 = gathered(a0, *shards(0), 0)
        h1 = h0 + dot(act0, d0, 1, 0).astype(BF)
        a1, back = jax.vjp(normed, h1)
        gu1, d1, act1, gate1, up1 = gathered(a1, *shards(1), 1)
        by_d1 = dot(act1, dy, 0, 0).astype(BF)
        mine_gu1, mine_d1, da = backward(a1, dy, d1, gate1, up1, by_d1, gu1, 2)
        dh = dy + back(da.astype(BF))[0]
        by_d0 = dot(act0, dh, 0, 0).astype(BF)
        mine_gu0, mine_d0 = backward(a0, dh, d0, gate0, up0, by_d0, None, 3)
        gradients = [jnp.stack([mine_gu0[n], mine_gu1[n]]).astype(F32) for n in (0, 1)] + [jnp.stack([mine_d0, mine_d1]).astype(F32)]
        squares = over_group(sum(jnp.sum(g * g) for g in gradients), 4)
        gradients = clipped(gradients, squares, S * sum(g.size for g in gradients))
        new = [adamw(w.astype(F32), m, v, g) for w, m, v, g in zip(weights, m, v, gradients, strict=True)]
        return tuple(one[which] for which in range(3) for one in new)

    states, cut = P(("rep", "r", "s"), None, None), P(None, "s", None)
    return jax.shard_map(
        step,
        mesh=mesh,
        in_specs=(states, states) + (cut,) * 9,
        out_specs=(P("rep", "s", None),) * 9,
        check_vma=False,
    )
```

```python
import functools

import jax
import jax.numpy as jnp
from jax import lax
from jax.experimental import pallas as pl
from jax.experimental.pallas import tpu as pltpu
from jax.sharding import PartitionSpec as P

NAMES = ("w_gate", "w_up", "w_down")
BF, F32 = jnp.bfloat16, jnp.float32
MESH = pl.DeviceIdType.MESH

TOKENS, D, FF = 2048, 1280, 4864
NY = NZ = NX = 4
S = NY * NZ * 2
RD, RF = D // S, FF // S
TF = 256
NT = FF // TF
ND = D // TF
VMEM_LIMIT = 67_000_000


def dot(a, b, ca, cb):
    return lax.dot_general(a, b, (((ca,), (cb,)), ((), ())), preferred_element_type=F32)


def at(*index):
    return index


def above(i):
    return i * ((i + 64) // 64)


def upto(i, last):
    return last - above(last - i)


def cols(start, size):
    return pl.ds(pl.multiple_of(start, 128), size)


class Place:
    def __init__(self):
        s = lax.axis_index("s")
        self.y, self.z, self.c = lax.div(s, NZ * 2), lax.rem(lax.div(s, 2), NZ), lax.rem(s, 2)
        self.x = lax.axis_index("r")
        self.pos = (self.y, self.z)

    def ring(self, axis, by):
        return lax.rem(self.pos[axis] + by, 4)

    def near(self, axis, by):
        y, z = (self.ring(0, by), self.z) if axis == 0 else (self.y, self.ring(1, by))
        return {"s": (y * NZ + z) * 2 + self.c}

    def partner(self):
        return {"s": (self.y * NZ + self.z) * 2 + 1 - self.c}

    def across(self, by):
        return {"r": lax.rem(self.x + by, NX)}

    def meet(self, x_too):
        barrier = pltpu.get_barrier_semaphore()
        peers = [self.near(axis, by) for axis in (0, 1) for by in (1, 3)] + [self.partner()]
        if x_too:
            peers += [self.across(by) for by in (1, 2, 3)]
        for peer in peers:
            pl.semaphore_signal(barrier, inc=1, device_id=peer, device_id_type=MESH)
        pl.semaphore_wait(barrier, len(peers))


def wait_bytes(ref, sem):
    pltpu.make_async_copy(ref, ref, sem).wait()


CH = NT + ND
LAG = 2
LEAD = 5 * LAG + 1


def gather_kernel(forward, *refs):
    if forward:
        a, wgu, wd, h, g_gu, g_d, act, gate, up, h_new, wt, wdt, act_s, ssem, rsem, lsem, osem = refs
    else:
        a, wgu, wd, dy, g_gu, g_d, gate, up, dwd, wt, act_s, ssem, rsem, lsem, osem = refs
    step = pl.program_id(0)
    i = step - LEAD
    me = Place()
    own = [
        pltpu.make_async_copy(wgu, g_gu.at[:, me.y, me.z, me.c], osem.at[0]),
        pltpu.make_async_copy(wd, g_d.at[me.y, me.z, me.c], osem.at[1]),
    ]

    @pl.when(step == 0)
    def _():
        me.meet(False)
        for copy in own:
            copy.start()

    @pl.when(step == 2 * LAG)
    def _():
        for copy in own:
            copy.wait()

    def block(kind, t, half, sub, y, z, c):
        width = TF if half is None else TF // 2
        start = t * TF + (half or 0) * (TF // 2)
        if kind == "gu":
            lead = slice(None) if sub is None else sub
            return g_gu.at[lead, y, z, c, :, cols(start, width)]
        rows = {None: slice(None), 0: pl.ds(0, 80), 1: pl.ds(80, RF - 80)}[sub]
        return g_d.at[y, z, c, rows, cols(start, width)]

    def mine(kind, t, half):
        start = t * TF + half * (TF // 2)
        return wgu.at[:, :, cols(start, TF // 2)] if kind == "gu" else wd.at[:, cols(start, TF // 2)]

    ALL = slice(None)

    def totals(kind, t, k):
        c = me.c
        y, z = [(pl.ds(0, 2), 0), (pl.ds(0, 1), 0), (ALL, pl.ds(0, 2)), (ALL, pl.ds(0, 1)), (ALL, ALL)][k]
        return block(kind, t, None, None, y, z, c)

    def send(kind, t, ch, k):
        def go(src, dst, peer):
            pltpu.make_async_remote_copy(
                src_ref=src, dst_ref=dst, send_sem=ssem.at[k, ch], recv_sem=rsem.at[k, ch], device_id=peer, device_id_type=MESH
            ).start()

        y, z, c = me.y, me.z, me.c
        for half in (0, 1):
            first, second = (0, 1) if half == 0 else (1, 0)
            if k == 0:
                for by in (1, 3):
                    go(mine(kind, t, half), block(kind, t, half, None, y, z, c), me.near(first, by))
            if k == 1:
                for sub, by in ((0, 1), (1, 3)):
                    back = me.ring(first, 4 - by)
                    ref = block(kind, t, half, sub, *((back, z) if first == 0 else (y, back)), c)
                    go(ref, ref, me.near(first, by))
            if k == 2:
                ref = block(kind, t, half, None, *((ALL, z) if first == 0 else (y, ALL)), c)
                for by in (1, 3):
                    go(ref, ref, me.near(second, by))
            if k == 3:
                for sub, by in ((0, 1), (1, 3)):
                    back = me.ring(second, 4 - by)
                    ref = block(kind, t, half, sub, *((ALL, back) if second == 1 else (back, ALL)), c)
                    go(ref, ref, me.near(second, by))
        if k == 4:
            ref = block(kind, t, None, None, ALL, ALL, c)
            go(ref, ref, me.partner())

    def load(kind, t):
        slot = lax.rem(t, 2)
        if kind == "gu":
            return pltpu.make_async_copy(g_gu.at[:, :, :, :, :, cols(t * TF, TF)], wt.at[slot], lsem.at[0, slot])
        return pltpu.make_async_copy(g_d.at[:, :, :, :, cols(t * TF, TF)], wdt.at[slot], lsem.at[1, slot])

    for k in (5, 4, 3, 2, 1, 0):
        ch = i + 1 + (5 - k) * LAG
        for kind, low, high in (("gu", 0, NT), ("d", NT, CH)):

            @pl.when((ch >= low) & (ch < high))
            def _(k=k, kind=kind, t=ch - low, ch=ch):
                if k > 0:
                    wait_bytes(totals(kind, t, k - 1), rsem.at[k - 1, ch])
                if k < 5:
                    send(kind, t, ch, k)
                elif kind == "gu" or forward:
                    load(kind, t).start()

    @pl.when((i >= 0) & (i < NT))
    def _():
        load("gu", i).wait()
        slot = lax.rem(i, 2)
        g = dot(a[...], wt[slot, 0].reshape(D, TF), 1, 0)
        u = dot(a[...], wt[slot, 1].reshape(D, TF), 1, 0)
        gate[...] = g
        up[...] = u
        hidden = (g * jax.nn.sigmoid(g) * u).astype(BF)
        if forward:
            act[...] = hidden
            act_s[:, cols(i * TF, TF)] = hidden
        else:
            act_s[...] = hidden
            dwd[...] = dot(act_s[...], dy[...], 0, 0).astype(BF)

    if forward:

        @pl.when(i >= NT)
        def _():
            load("d", i - NT).wait()
            h_new[...] = h[...] + dot(act_s[...], wdt[lax.rem(i - NT, 2)].reshape(FF, TF), 1, 0).astype(BF)

    @pl.when(step == LEAD + CH - 1)
    def _():
        for k in range(5):
            for kind, low, high in (("gu", 0, NT), ("d", NT, CH)):

                @pl.loop(low, high)
                def _(ch, k=k, kind=kind, low=low):
                    wait_bytes(totals(kind, ch - low, k), ssem.at[k, ch])


def gathered(a, wgu, wd, other, number):
    forward = number == 0
    vmem, hbm = pl.BlockSpec(memory_space=pltpu.VMEM), pl.BlockSpec(memory_space=pl.ANY)
    tile = pl.BlockSpec((TOKENS, TF), lambda step: (0, upto(above(step - LEAD), NT - 1)))
    column = pl.BlockSpec((TOKENS, TF), lambda step: (0, above(step - LEAD - NT)))
    row = pl.BlockSpec((TF, D), lambda step: (upto(above(step - LEAD), NT - 1), 0))
    shape = jax.ShapeDtypeStruct
    wide = [shape((TOKENS, FF), F32)] * 2
    g_gu, g_d, *rest = pl.pallas_call(
        functools.partial(gather_kernel, forward),
        grid=(LEAD + CH,),
        in_specs=[vmem, vmem, vmem, column if forward else vmem],
        out_specs=[hbm, hbm, *([tile] * 3 + [column] if forward else [tile, tile, row])],
        out_shape=[
            shape((2, NY, NZ, 2, RD, FF), BF),
            shape((NY, NZ, 2, RF, D), BF),
            *([shape((TOKENS, FF), BF), *wide, shape((TOKENS, D), BF)] if forward else [*wide, shape((FF, D), BF)]),
        ],
        scratch_shapes=[
            pltpu.VMEM((2, 2, NY, NZ, 2, RD, TF), BF),
            *([pltpu.VMEM((2, NY, NZ, 2, RF, TF), BF), pltpu.VMEM((TOKENS, FF), BF)] if forward else [pltpu.VMEM((TOKENS, TF), BF)]),
            pltpu.SemaphoreType.DMA((5, CH)),
            pltpu.SemaphoreType.DMA((5, CH)),
            pltpu.SemaphoreType.DMA((2, 2)),
            pltpu.SemaphoreType.DMA((2,)),
        ],
        compiler_params=pltpu.CompilerParams(
            collective_id=number, has_side_effects=True, vmem_limit_bytes=VMEM_LIMIT, dimension_semantics=("arbitrary",)
        ),
        cost_estimate=pl.CostEstimate(flops=6 * TOKENS * D * FF, bytes_accessed=200_000_000, transcendentals=TOKENS * FF),
        name=f"gather_{number}",
    )(a, wgu, wd, other)
    return g_gu.reshape(2, D, FF), g_d.reshape(FF, D), *rest


DC = 128
NDC = D // DC


class Summing:
    HEIGHTS = {"gu": ((RD, RD), (RD, RD)), "d": ((40, 40), (40, RF - 120))}

    def __init__(self, kind, count, stride, lag, me, own, inbox, s1, r2, s2, r3, acc, s4, r4, s5, r5, xb, ssem, rsem, out):
        self.kind, self.count, self.stride, self.lag, self.me = kind, count, stride, lag, me
        self.big, self.small, self.sent = slots(stride, lag)
        self.own, self.inbox, self.s1, self.r2, self.s2, self.r3 = own, inbox, s1, r2, s2, r3
        self.acc, self.s4, self.r4, self.s5, self.r5, self.xb = acc, s4, r4, s5, r5, xb
        self.ssem, self.rsem, self.out = ssem, rsem, out
        self.subs = (slice(None),) if kind == "gu" else (0, 1)

    def due(self, i, k):
        passed = i - 1 - k * self.lag
        t = lax.div(passed, self.stride)
        return t, (passed >= 0) & (t < self.count) & (lax.rem(passed, self.stride) == 0)

    def part(self, half, sub):
        if self.kind == "gu":
            return sub, slice(None), pl.ds(half * 128, 128)
        low = 80 * half + 40 * sub
        return 0, pl.ds(low, self.HEIGHTS["d"][half][sub]), slice(None)

    def rows(self, half, sub):
        return slice(None) if self.kind == "gu" else pl.ds(0, self.HEIGHTS["d"][half][sub])

    def both(self, slot, y, z, half, sub):
        lead, rows, columns = self.part(half, sub)
        mine = self.own[slot, lead, y, z, self.me.c, rows, columns] if self.kind == "gu" else self.own[slot, y, z, rows, columns]
        theirs = self.inbox[slot, lead, y, z, rows, columns] if self.kind == "gu" else self.inbox[slot, y, z, rows, columns]
        return mine.astype(F32) + theirs.astype(F32)

    def size(self, k, slot, two):
        if k == 0:
            return self.inbox.at[slot]
        if k == 5:
            return self.xb.at[two, pl.ds(0, 3)]
        if self.kind == "gu":
            return (self.r2, self.r3, self.r4, self.r5)[k - 1].at[two]
        return self.inbox.at[(slot, *((0,), (pl.ds(0, 2),), (0, 0), (0, pl.ds(0, 2)))[k - 1])]

    def compute(self, k, t):
        me, slot, two, sent = self.me, lax.rem(t, self.big), lax.rem(t, self.small), lax.rem(t, self.sent)
        if k > 0:
            wait_bytes(self.size(k - 1, slot, two), self.rsem.at[k - 1, slot])
            wait_bytes(self.size(k - 1, slot, two), self.ssem.at[k - 1, slot])
        if k == 6:
            total = self.xb[two, 0].astype(F32)
            for x in range(1, NX):
                total = total + self.xb[two, x].astype(F32)
            if self.kind == "gu":
                self.out[:, :, cols(t * TF, TF)] = total.astype(BF)
            else:
                self.out[:, cols(t * DC, DC)] = total.astype(BF)
            return
        for half in (0, 1):
            first, second = (0, 1) if half == 0 else (1, 0)
            along = lambda place: (place, slice(None)) if first == 0 else (slice(None), place)
            for sub in (0, 1):
                rows = self.rows(half, sub)
                if k == 1:
                    self.s1[sent, half, sub, :, rows] = self.both(slot, *along(me.ring(first, 2)), half, sub).astype(BF)
                if k == 2:
                    for way, by in ((0, 1), (1, 3)):
                        term = self.both(slot, *along(me.ring(first, by)), half, sub)
                        if sub == way:
                            term = term + self.r2[two, half, sub, :, rows].astype(F32)
                        self.s2[sent, half, way, sub, :, rows] = term.astype(BF)
                if k == 3:
                    term = self.both(slot, *along(me.pos[first]), half, sub)
                    for way in (0, 1):
                        term = term + self.r3[two, half, way, sub, :, rows].astype(F32)
                    self.acc[two, half, sub, :, rows] = term
                    self.s4[sent, half, sub, rows] = self.acc[two, half, sub, me.ring(second, 2), rows].astype(BF)
                if k == 4:
                    for way, by in ((0, 1), (1, 3)):
                        term = self.acc[two, half, sub, me.ring(second, by), rows]
                        if sub == way:
                            term = term + self.r4[two, half, sub, rows].astype(F32)
                        self.s5[sent, half, way, sub, rows] = term.astype(BF)
                if k == 5:
                    term = self.acc[two, half, sub, me.pos[second], rows]
                    for way in (0, 1):
                        term = term + self.r5[two, half, way, sub, rows].astype(F32)
                    lead, where, columns = self.part(half, sub)
                    if self.kind == "gu":
                        self.xb[two, me.x, lead, where, columns] = term.astype(BF)
                    else:
                        self.xb[two, me.x, where, columns] = term.astype(BF)

    def send(self, k, t, source=None):
        me, slot, two, sent = self.me, lax.rem(t, self.big), lax.rem(t, self.small), lax.rem(t, self.sent)

        def go(src, dst, peer):
            pltpu.make_async_remote_copy(
                src_ref=src, dst_ref=dst, send_sem=self.ssem.at[k, slot], recv_sem=self.rsem.at[k, slot], device_id=peer, device_id_type=MESH
            ).start()

        if k == 0:
            go(source, self.inbox.at[slot], me.partner())
        if k == 5:
            for by in (1, 2, 3):
                go(self.xb.at[two, me.x], self.xb.at[two, me.x], me.across(by))
        for half in (0, 1):
            first, second = (0, 1) if half == 0 else (1, 0)
            for way, by in ((0, 1), (1, 3)):
                if k == 1:
                    rows = self.rows(half, way)
                    go(self.s1.at[sent, half, way, :, rows], self.r2.at[two, half, way, :, rows], me.near(first, by))
                if k == 3:
                    rows = self.rows(half, way)
                    go(self.s4.at[sent, half, way, rows], self.r4.at[two, half, way, rows], me.near(second, by))
                if k in (2, 4):
                    for sub in self.subs:
                        rows = self.rows(half, sub)
                        if k == 2:
                            go(self.s2.at[sent, half, way, sub, :, rows], self.r3.at[two, half, way, sub, :, rows], me.near(first, by))
                        else:
                            go(self.s5.at[sent, half, way, sub, rows], self.r5.at[two, half, way, sub, rows], me.near(second, by))


def slots(stride, lag):
    return -(-4 * lag // stride), -(-2 * lag // stride), -(-lag // stride)


def stage_buffers(kind, stride, lag):
    block = (2, NY, NZ, RD, TF) if kind == "gu" else (NY, NZ, RF, DC)
    last = (2, RD, TF) if kind == "gu" else (RF, DC)
    big, small, sent = slots(stride, lag)
    return [
        pltpu.VMEM((big, 2, NY, NZ, 2, RD, TF) if kind == "gu" else (big, *block), BF),
        pltpu.VMEM((big, *block), BF),
        pltpu.VMEM((sent, 2, 2, 4, 40, 128), BF),
        pltpu.VMEM((small, 2, 2, 4, 40, 128), BF),
        pltpu.VMEM((sent, 2, 2, 2, 4, 40, 128), BF),
        pltpu.VMEM((small, 2, 2, 2, 4, 40, 128), BF),
        pltpu.VMEM((small, 2, 2, 4, 40, 128), F32),
        pltpu.VMEM((sent, 2, 2, 40, 128), BF),
        pltpu.VMEM((small, 2, 2, 40, 128), BF),
        pltpu.VMEM((sent, 2, 2, 2, 40, 128), BF),
        pltpu.VMEM((small, 2, 2, 2, 40, 128), BF),
        pltpu.VMEM((small, NX, *last), BF),
        pltpu.SemaphoreType.DMA((6, big)),
        pltpu.SemaphoreType.DMA((6, big)),
    ]


NBUF = 14


def pace(with_da):
    return (1, 1) if with_da else (2, 2)


def back_kernel(with_da, *refs):
    refs = list(refs)
    take = lambda n: [refs.pop(0) for _ in range(n)]
    a, dy, wd, gate, up, dwd = take(6)
    wgu = take(1)[0] if with_da else None
    out_gu, out_d = take(2)
    da = take(1)[0] if with_da else None
    gu_bufs, d_bufs = take(NBUF), take(NBUF)
    dgu_s, lsem = take(2)
    i = pl.program_id(0)
    me = Place()

    @pl.when(i == 0)
    def _():
        me.meet(True)

    own = gu_bufs[0]
    lag, stride = pace(with_da)
    gu = Summing("gu", NT, 1, lag, me, *gu_bufs, out_gu)
    down = Summing("d", NDC, stride, lag, me, *d_bufs, out_d)

    def load(n):
        slot = lax.rem(n, down.big)
        return pltpu.make_async_copy(dwd.at[:, :, me.c, :, cols(n * DC, DC)], down.own.at[slot], lsem.at[slot])

    for k in (6, 5, 4, 3, 2, 1):
        for engine in (gu, down):
            t, there = engine.due(i, k)

            @pl.when(there)
            def _(k=k, engine=engine, t=t):
                if k == 1 and engine is down:
                    load(t).wait()
                engine.compute(k, t)

    for k in (5, 4, 3, 2, 1, 0):
        for engine in (gu, down):
            t, there = engine.due(i, k)

            @pl.when(there)
            def _(k=k, engine=engine, t=t):
                source = None
                if k == 0:
                    source = own.at[lax.rem(t, gu.big), :, :, :, 1 - me.c] if engine is gu else dwd.at[:, :, 1 - me.c, :, cols(t * DC, DC)]
                engine.send(k, t, source)

    @pl.when((i < NDC * stride) & (lax.rem(i, stride) == 0))
    def _():
        load(lax.div(i, stride)).start()

    @pl.when(i < NT)
    def _():
        slot = lax.rem(i, gu.big)
        dh = dot(dy[...], wd[...], 1, 1).astype(BF).astype(F32)
        g, u = gate[...], up[...]
        sg = jax.nn.sigmoid(g)
        dgu_s[:, TF:] = (dh * (g * sg)).astype(BF)
        dgu_s[:, :TF] = (dh * u * (sg * (1 + g * (1 - sg)))).astype(BF)
        own[slot, 0] = dot(a[...], dgu_s[:, :TF], 0, 0).reshape(NY, NZ, 2, RD, TF).astype(BF)
        own[slot, 1] = dot(a[...], dgu_s[:, TF:], 0, 0).reshape(NY, NZ, 2, RD, TF).astype(BF)
        if with_da:
            more = dot(dgu_s[...], jnp.concatenate([wgu[0], wgu[1]], 1), 1, 1)

            @pl.when(i == 0)
            def _():
                da[...] = more

            @pl.when(i > 0)
            def _():
                da[...] += more


def backward(a, dy, g_d, gate, up, dwd, g_gu, number):
    with_da = g_gu is not None
    lag, stride = pace(with_da)
    last = lambda i: upto(i, NT - 1)
    vmem, hbm = pl.BlockSpec(memory_space=pltpu.VMEM), pl.BlockSpec(memory_space=pl.ANY)
    tile = pl.BlockSpec((TOKENS, TF), lambda i: (0, last(i)))
    in_specs = [vmem, vmem, pl.BlockSpec((TF, D), lambda i: (last(i), 0)), tile, tile, hbm]
    out_shape = [jax.ShapeDtypeStruct((2, RD, FF), BF), jax.ShapeDtypeStruct((RF, D), BF)]
    operands = [a, dy, g_d, gate, up, dwd.reshape(NY, NZ, 2, RF, D)]
    if with_da:
        in_specs.append(pl.BlockSpec((2, D, TF), lambda i: (0, 0, last(i))))
        out_shape.append(jax.ShapeDtypeStruct((TOKENS, D), F32))
        operands.append(g_gu)
    return pl.pallas_call(
        functools.partial(back_kernel, with_da),
        grid=(NT + 1 + 6 * lag,),
        in_specs=in_specs,
        out_specs=[vmem] * len(out_shape),
        out_shape=out_shape,
        scratch_shapes=[
            *stage_buffers("gu", 1, lag),
            *stage_buffers("d", stride, lag),
            pltpu.VMEM((TOKENS, 2 * TF), BF),
            pltpu.SemaphoreType.DMA((slots(stride, lag)[0],)),
        ],
        compiler_params=pltpu.CompilerParams(
            collective_id=number, has_side_effects=True, vmem_limit_bytes=VMEM_LIMIT, dimension_semantics=("arbitrary",)
        ),
        cost_estimate=pl.CostEstimate(
            flops=(10 if with_da else 6) * TOKENS * D * FF, bytes_accessed=200_000_000, transcendentals=TOKENS * FF
        ),
        name=f"backward_{number}",
    )(*operands)


def total_kernel(part, out, b0, b1, b2, ssem, rsem):
    me = Place()
    barrier = pltpu.get_barrier_semaphore()
    rings = [[me.near(axis, by) for by in (1, 2, 3)] for axis in (0, 1)] + [[me.partner()]]
    peers = [peer for ring in rings for peer in ring]
    for peer in peers:
        pl.semaphore_signal(barrier, inc=1, device_id=peer, device_id_type=MESH)
    pl.semaphore_wait(barrier, len(peers))
    value = part[...]
    for k, (buf, place, ring) in enumerate(zip((b0, b1, b2), (me.y, me.z, me.c), rings, strict=True)):
        buf[place] = value
        for peer in ring:
            pltpu.make_async_remote_copy(
                src_ref=buf.at[place], dst_ref=buf.at[place], send_sem=ssem.at[k], recv_sem=rsem.at[k], device_id=peer, device_id_type=MESH
            ).start()
        wait_bytes(buf.at[pl.ds(0, len(ring))], rsem.at[k])
        wait_bytes(buf.at[pl.ds(0, len(ring))], ssem.at[k])
        value = buf[0]
        for n in range(1, len(ring) + 1):
            value = value + buf[n]
    out[...] = value


def over_group(number, collective):
    part = jnp.full((8, 128), number, F32)
    vmem = pl.BlockSpec(memory_space=pltpu.VMEM)
    out = pl.pallas_call(
        total_kernel,
        in_specs=[vmem],
        out_specs=vmem,
        out_shape=jax.ShapeDtypeStruct((8, 128), F32),
        scratch_shapes=[
            pltpu.VMEM((NY, 8, 128), F32),
            pltpu.VMEM((NZ, 8, 128), F32),
            pltpu.VMEM((2, 8, 128), F32),
            pltpu.SemaphoreType.DMA((3,)),
            pltpu.SemaphoreType.DMA((3,)),
        ],
        compiler_params=pltpu.CompilerParams(collective_id=collective, has_side_effects=True),
        name="total",
    )(part)
    return out[0, 0]


def normed(h):
    wide = h.astype(F32)
    scale = lax.rsqrt(jnp.mean(wide**2, -1, keepdims=True) + 1e-6)
    return (wide * scale).astype(BF)


def adamw(w, m, v, g):
    m = 0.9 * m + 0.1 * g
    v = 0.95 * v + 0.05 * g * g
    step = m * lax.rsqrt(v + 1e-8) + 0.1 * w
    return (w - 0.02 * step).astype(BF), m, v


def clipped(gradients, sum_of_squares, count):
    factor = jnp.minimum(1.0, 0.5 * lax.rsqrt(sum_of_squares / count + 1e-30))
    return [g * factor for g in gradients]


def solution(mesh):
    def step(x, dy, *arrays):
        weights, m, v = (arrays[i : i + 3] for i in (0, 3, 6))
        shards = lambda layer: (jnp.stack([weights[0][layer], weights[1][layer]]), weights[2][layer])
        h0, dy = x[0], dy[0]
        a0 = normed(h0)
        _, d0, act0, gate0, up0, h1 = gathered(a0, *shards(0), h0, 0)
        a1, back = jax.vjp(normed, h1)
        gu1, d1, gate1, up1, by_d1 = gathered(a1, *shards(1), dy, 1)
        mine_gu1, mine_d1, da = backward(a1, dy, d1, gate1, up1, by_d1, gu1, 2)
        dh = dy + back(da.astype(BF))[0]
        by_d0 = dot(act0, dh, 0, 0).astype(BF)
        mine_gu0, mine_d0 = backward(a0, dh, d0, gate0, up0, by_d0, None, 3)
        gradients = [jnp.stack([mine_gu0[n], mine_gu1[n]]).astype(F32) for n in (0, 1)] + [jnp.stack([mine_d0, mine_d1]).astype(F32)]
        squares = over_group(sum(jnp.sum(g * g) for g in gradients), 4)
        gradients = clipped(gradients, squares, S * sum(g.size for g in gradients))
        new = [adamw(w.astype(F32), m, v, g) for w, m, v, g in zip(weights, m, v, gradients, strict=True)]
        return tuple(one[which] for which in range(3) for one in new)

    states, cut = P(("rep", "r", "s"), None, None), P(None, "s", None)
    return jax.shard_map(
        step,
        mesh=mesh,
        in_specs=(states, states) + (cut,) * 9,
        out_specs=(P("rep", "s", None),) * 9,
        check_vma=False,
    )
```

```python
import functools

import jax
import jax.numpy as jnp
from jax import lax
from jax.experimental import pallas as pl
from jax.experimental.pallas import tpu as pltpu
from jax.sharding import PartitionSpec as P

NAMES = ("w_gate", "w_up", "w_down")
BF, F32 = jnp.bfloat16, jnp.float32
MESH = pl.DeviceIdType.MESH

TOKENS, D, FF = 2048, 1280, 4864
NY = NZ = NX = 4
S = NY * NZ * 2
RD, RF = D // S, FF // S
TF = 256
NT = FF // TF
ND = D // TF
VMEM_LIMIT = 67_000_000
AXES = ((0, 1), (1, 0))
WAYS = ((0, 1), (1, 3))


def dot(a, b, ca, cb):
    return lax.dot_general(a, b, (((ca,), (cb,)), ((), ())), preferred_element_type=F32)


def at(*index):
    return index


def above(i):
    return i * ((i + 64) // 64)


def upto(i, last):
    return last - above(last - i)


def cols(start, size):
    return pl.ds(pl.multiple_of(start, 128), size)


class Place:
    def __init__(self):
        s = lax.axis_index("s")
        self.y, self.z, self.c = lax.div(s, NZ * 2), lax.rem(lax.div(s, 2), NZ), lax.rem(s, 2)
        self.x = lax.axis_index("r")
        self.pos = (self.y, self.z)

    def ring(self, axis, by):
        return lax.rem(self.pos[axis] + by, 4)

    def near(self, axis, by):
        y, z = (self.ring(0, by), self.z) if axis == 0 else (self.y, self.ring(1, by))
        return {"s": (y * NZ + z) * 2 + self.c}

    def partner(self):
        return {"s": (self.y * NZ + self.z) * 2 + 1 - self.c}

    def across(self, by):
        return {"r": lax.rem(self.x + by, NX)}

    def meet(self, x_too):
        barrier = pltpu.get_barrier_semaphore()
        peers = [self.near(axis, by) for axis in (0, 1) for by in (1, 3)] + [self.partner()]
        if x_too:
            peers += [self.across(by) for by in (1, 2, 3)]
        for peer in peers:
            pl.semaphore_signal(barrier, inc=1, device_id=peer, device_id_type=MESH)
        pl.semaphore_wait(barrier, len(peers))


def wait_bytes(ref, sem):
    pltpu.make_async_copy(ref, ref, sem).wait()


CH = NT + 2
LAG = 2
LEAD = 5 * LAG + 1
STAGES = 7
ALONG_X = (-7, -5, -3, -1, 1, 9, 13, NT - 1)
WITHIN = (3, 5, 7, 9, None, None, 11, NT - 1)


def gather_kernel(forward, *refs):
    if forward:
        h, wgu, wd, g_gu, g_d, a_out, act, gate, up, h_new, wt, wdt, act_s, a, ssem, rsem, lsem, osem = refs
    else:
        h, wgu, wd, dy, g_gu, g_d, a_out, gate, up, dwd, wt, act_s, a, ssem, rsem, lsem, osem = refs
    step = pl.program_id(0)
    i = step - LEAD
    me = Place()
    own = [
        pltpu.make_async_copy(wgu, g_gu.at[:, me.y, me.z, me.c], osem.at[0]),
        *(
            pltpu.make_async_copy(wd.at[:, cols(t * TF, TF)], g_d.at[me.y, me.z, me.c, :, cols(t * TF, TF)], osem.at[n])
            for n, t in ((1, me.x), (2, ND - 1))
        ),
    ]

    @pl.when(step == 0)
    def _():
        me.meet(True)
        for copy in own:
            copy.start()

    @pl.when(step == 2 * LAG)
    def _():
        for copy in own:
            copy.wait()

    def block(kind, t, half, sub, y, z, c):
        width = TF if half is None else TF // 2
        start = t * TF + (half or 0) * (TF // 2)
        if kind == "gu":
            lead = slice(None) if sub is None else sub
            return g_gu.at[lead, y, z, c, :, cols(start, width)]
        rows = {None: slice(None), 0: pl.ds(0, 80), 1: pl.ds(80, RF - 80)}[sub]
        return g_d.at[y, z, c, rows, cols(start, width)]

    def mine(kind, t, half):
        start = t * TF + half * (TF // 2)
        return wgu.at[:, :, cols(start, TF // 2)] if kind == "gu" else wd.at[:, cols(start, TF // 2)]

    ALL = slice(None)

    def cores(kind, t, c):
        return g_d.at[:, :, c, :, 0 : NX * TF] if kind == "x" else block(kind, t, None, None, ALL, ALL, c)

    def totals(kind, t, k):
        c = me.c
        if k == 6:
            return cores(kind, t, c)
        y, z, c = [(pl.ds(0, 2), 0, c), (pl.ds(0, 1), 0, c), (ALL, pl.ds(0, 2), c), (ALL, pl.ds(0, 1), c), (ALL, ALL, ALL), (ALL, ALL, c)][k]
        return block(kind, t, None, None, y, z, c)

    def send(kind, t, ch, k):
        def go(src, dst, peer):
            pltpu.make_async_remote_copy(
                src_ref=src, dst_ref=dst, send_sem=ssem.at[k, ch], recv_sem=rsem.at[k, ch], device_id=peer, device_id_type=MESH
            ).start()

        y, z, c = me.y, me.z, me.c
        if k < 4:
            for half in (0, 1):
                first, second = AXES[half]
                if k == 0:
                    for by in (1, 3):
                        go(mine(kind, t, half), block(kind, t, half, None, y, z, c), me.near(first, by))
                if k == 1:
                    for sub, by in WAYS:
                        back = me.ring(first, 4 - by)
                        ref = block(kind, t, half, sub, *((back, z) if first == 0 else (y, back)), c)
                        go(ref, ref, me.near(first, by))
                if k == 2:
                    ref = block(kind, t, half, None, *((ALL, z) if first == 0 else (y, ALL)), c)
                    for by in (1, 3):
                        go(ref, ref, me.near(second, by))
                if k == 3:
                    for sub, by in WAYS:
                        back = me.ring(second, 4 - by)
                        ref = block(kind, t, half, sub, *((ALL, back) if second == 1 else (back, ALL)), c)
                        go(ref, ref, me.near(second, by))
        if k == 4:
            ref = block(kind, t, None, None, ALL, ALL, c)
            for by in (1, 3):
                go(ref, ref, me.across(by))
        if k == 5:
            for sub, by in WAYS:
                ref = block(kind, lax.rem(me.x + 4 - by, NX), None, sub, ALL, ALL, c)
                go(ref, ref, me.across(by))
        if k == 6:
            ref = cores(kind, t, c)
            go(ref, ref, me.partner())

    def load(kind, t):
        slot = lax.rem(t, 2)
        if kind == "gu":
            return pltpu.make_async_copy(g_gu.at[:, :, :, :, :, cols(t * TF, TF)], wt.at[slot], lsem.at[0, slot])
        return pltpu.make_async_copy(g_d.at[:, :, :, :, cols(t * TF, TF)], wdt.at[slot], lsem.at[1, slot])

    PLANE = (0, 1, 2, 3, 6)

    save = pltpu.make_async_copy(a, a_out, osem.at[3])

    @pl.when(step == 1)
    def _():
        rows = TOKENS // 4
        for r in range(4):
            part = pl.ds(r * rows, rows)
            a[part, :] = normed(h[part, :])

    @pl.when(step == 2)
    def _():
        save.start()

    for n in (5, 4, 3, 2, 1, 0):
        t = i + 1 + (5 - n) * LAG

        @pl.when((t >= 0) & (t < NT))
        def _(n=n, t=t):
            if n > 0:
                wait_bytes(totals("gu", t, PLANE[n - 1]), rsem.at[PLANE[n - 1], t])
            if n < 5:
                send("gu", t, t, PLANE[n])
            else:
                load("gu", t).start()

    for kind, t, ch, due in (("x", me.x, NT, ALONG_X), ("d", ND - 1, NT + 1, WITHIN)):
        stages = [k for k in range(STAGES + 1) if due[k] is not None]
        for before, k in zip([None, *stages], stages):

            @pl.when(i == due[k])
            def _(kind=kind, t=t, ch=ch, before=before, k=k):
                if before is not None:
                    wait_bytes(totals(kind, t, before), rsem.at[before, ch])
                if k < STAGES:
                    send(kind, t, ch, k)

    if forward:

        @pl.when((i >= NT - 1) & (i < NT + ND - 1))
        def _():
            load("d", i - NT + 1).start()

    @pl.when((i >= 0) & (i < NT))
    def _():
        load("gu", i).wait()
        slot = lax.rem(i, 2)
        g = dot(a[...], wt[slot, 0].reshape(D, TF), 1, 0)
        u = dot(a[...], wt[slot, 1].reshape(D, TF), 1, 0)
        gate[...] = g
        up[...] = u
        hidden = (g * jax.nn.sigmoid(g) * u).astype(BF)
        if forward:
            act[...] = hidden
            act_s[:, cols(i * TF, TF)] = hidden
        else:
            act_s[...] = hidden
            dwd[...] = dot(act_s[...], dy[...], 0, 0).astype(BF)

    if forward:

        @pl.when(i >= NT)
        def _():
            load("d", i - NT).wait()
            h_new[...] = h[:, cols((i - NT) * TF, TF)] + dot(act_s[...], wdt[lax.rem(i - NT, 2)].reshape(FF, TF), 1, 0).astype(BF)

    @pl.when(step == pl.num_programs(0) - 1)
    def _():
        save.wait()
        for k in PLANE:

            @pl.loop(0, NT)
            def _(t, k=k):
                wait_bytes(totals("gu", t, k), ssem.at[k, t])

        for kind, t, ch, due in (("x", me.x, NT, ALONG_X), ("d", ND - 1, NT + 1, WITHIN)):
            for k in range(STAGES):
                if due[k] is not None:
                    wait_bytes(totals(kind, t, k), ssem.at[k, ch])


def gathered(h, wgu, wd, dy, number):
    forward = dy is None
    vmem, hbm = pl.BlockSpec(memory_space=pltpu.VMEM), pl.BlockSpec(memory_space=pl.ANY)
    tile = pl.BlockSpec((TOKENS, TF), lambda step: (0, upto(above(step - LEAD), NT - 1)))
    column = pl.BlockSpec((TOKENS, TF), lambda step: (0, above(step - LEAD - NT)))
    row = pl.BlockSpec((TF, D), lambda step: (upto(above(step - LEAD), NT - 1), 0))
    shape, sems = jax.ShapeDtypeStruct, pltpu.SemaphoreType.DMA
    wide = [shape((TOKENS, FF), F32)] * 2
    states = shape((TOKENS, D), BF)
    g_gu, g_d, *rest = pl.pallas_call(
        functools.partial(gather_kernel, forward),
        grid=(LEAD + NT + (ND if forward else 0),),
        in_specs=[vmem, vmem, vmem] + ([] if forward else [vmem]),
        out_specs=[hbm, hbm, hbm, *([tile] * 3 + [column] if forward else [tile, tile, row])],
        out_shape=[
            shape((2, NY, NZ, 2, RD, FF), BF),
            shape((NY, NZ, 2, RF, D), BF),
            states,
            *([shape((TOKENS, FF), BF), *wide, states] if forward else [*wide, shape((FF, D), BF)]),
        ],
        scratch_shapes=[
            pltpu.VMEM((2, 2, NY, NZ, 2, RD, TF), BF),
            *([pltpu.VMEM((2, NY, NZ, 2, RF, TF), BF), pltpu.VMEM((TOKENS, FF), BF)] if forward else [pltpu.VMEM((TOKENS, TF), BF)]),
            pltpu.VMEM((TOKENS, D), BF),
            sems((STAGES, CH)),
            sems((STAGES, CH)),
            sems((2, 2)),
            sems((4,)),
        ],
        compiler_params=pltpu.CompilerParams(
            collective_id=number, has_side_effects=True, vmem_limit_bytes=VMEM_LIMIT, dimension_semantics=("arbitrary",)
        ),
        cost_estimate=pl.CostEstimate(flops=6 * TOKENS * D * FF, bytes_accessed=200_000_000, transcendentals=TOKENS * FF),
        name=f"gather_{number}",
    )(h, wgu, wd, *([] if forward else [dy]))
    return g_gu.reshape(2, D, FF), g_d.reshape(FF, D), *rest


DC = 128
STRIDE = {"gu": 1, "d": 2}
BIG, SMALL = {"gu": 4, "d": 2}, 2
NR = 8
NDC = D // DC


class Summing:
    HEIGHTS = {"gu": ((RD, RD), (RD, RD)), "d": ((40, 40), (40, RF - 120))}

    def __init__(self, kind, count, me, own, inbox, s1, r2, s2, r3, acc, s4, r4, s5, r5, xb, ssem, rsem, out):
        self.kind, self.count, self.me = kind, count, me
        self.stride, self.big = STRIDE[kind], BIG[kind]
        self.own, self.inbox, self.s1, self.r2, self.s2, self.r3 = own, inbox, s1, r2, s2, r3
        self.acc, self.s4, self.r4, self.s5, self.r5, self.xb = acc, s4, r4, s5, r5, xb
        self.ssem, self.rsem, self.out = ssem, rsem, out
        self.subs = (slice(None),) if kind == "gu" else (0, 1)

    def due(self, i, k):
        passed = i - 1 - k
        t = lax.div(passed, self.stride)
        return t, (passed >= 0) & (t < self.count) & (lax.rem(passed, self.stride) == 0)

    def part(self, half, sub):
        if self.kind == "gu":
            return sub, slice(None), pl.ds(half * 128, 128)
        low = 80 * half + 40 * sub
        return 0, pl.ds(low, self.HEIGHTS["d"][half][sub]), slice(None)

    def rows(self, half, sub):
        return slice(None) if self.kind == "gu" else pl.ds(0, self.HEIGHTS["d"][half][sub])

    def both(self, slot, y, z, half, sub):
        lead, rows, columns = self.part(half, sub)
        mine = self.own[slot, lead, y, z, self.me.c, rows, columns] if self.kind == "gu" else self.own[slot, y, z, rows, columns]
        theirs = self.inbox[slot, lead, y, z, rows, columns] if self.kind == "gu" else self.inbox[slot, y, z, rows, columns]
        return mine.astype(F32) + theirs.astype(F32)

    def size(self, k, slot, two):
        if k == 0:
            return self.inbox.at[slot]
        if k == 5:
            return self.xb.at[two, pl.ds(0, 3)]
        if self.kind == "gu":
            return (self.r2, self.r3, self.r4, self.r5)[k - 1].at[two]
        return self.inbox.at[(slot, *((0,), (pl.ds(0, 2),), (0, 0), (0, pl.ds(0, 2)))[k - 1])]

    def compute(self, k, t):
        me, slot, two = self.me, lax.rem(t, self.big), lax.rem(t, SMALL)
        if k > 0:
            wait_bytes(self.size(k - 1, slot, two), self.rsem.at[k - 1, slot])
            wait_bytes(self.size(k - 1, slot, two), self.ssem.at[k - 1, slot])
        if k == 6:
            total = self.xb[two, 0].astype(F32)
            for x in range(1, NX):
                total = total + self.xb[two, x].astype(F32)
            if self.kind == "gu":
                self.out[:, :, cols(t * TF, TF)] = total.astype(BF)
            else:
                self.out[:, cols(t * DC, DC)] = total.astype(BF)
            return
        for half in (0, 1):
            first, second = AXES[half]
            along = lambda place: (place, slice(None)) if first == 0 else (slice(None), place)
            for sub in (0, 1):
                rows = self.rows(half, sub)
                if k == 1:
                    self.s1[half, sub, :, rows] = self.both(slot, *along(me.ring(first, 2)), half, sub).astype(BF)
                if k == 2:
                    for way, by in WAYS:
                        term = self.both(slot, *along(me.ring(first, by)), half, sub)
                        if sub == way:
                            term = term + self.r2[two, half, sub, :, rows].astype(F32)
                        self.s2[half, way, sub, :, rows] = term.astype(BF)
                if k == 3:
                    term = self.both(slot, *along(me.pos[first]), half, sub)
                    for way in (0, 1):
                        term = term + self.r3[two, half, way, sub, :, rows].astype(F32)
                    self.acc[two, half, sub, :, rows] = term
                    self.s4[half, sub, rows] = self.acc[two, half, sub, me.ring(second, 2), rows].astype(BF)
                if k == 4:
                    for way, by in WAYS:
                        term = self.acc[two, half, sub, me.ring(second, by), rows]
                        if sub == way:
                            term = term + self.r4[two, half, sub, rows].astype(F32)
                        self.s5[half, way, sub, rows] = term.astype(BF)
                if k == 5:
                    term = self.acc[two, half, sub, me.pos[second], rows]
                    for way in (0, 1):
                        term = term + self.r5[two, half, way, sub, rows].astype(F32)
                    lead, where, columns = self.part(half, sub)
                    if self.kind == "gu":
                        self.xb[two, me.x, lead, where, columns] = term.astype(BF)
                    else:
                        self.xb[two, me.x, where, columns] = term.astype(BF)

    def send(self, k, t, source=None):
        me, slot, two = self.me, lax.rem(t, self.big), lax.rem(t, SMALL)

        def go(src, dst, peer):
            pltpu.make_async_remote_copy(
                src_ref=src, dst_ref=dst, send_sem=self.ssem.at[k, slot], recv_sem=self.rsem.at[k, slot], device_id=peer, device_id_type=MESH
            ).start()

        if k == 0:
            go(source, self.inbox.at[slot], me.partner())
        if k == 5:
            for by in (1, 2, 3):
                go(self.xb.at[two, me.x], self.xb.at[two, me.x], me.across(by))
        for half in (0, 1):
            first, second = AXES[half]
            for way, by in WAYS:
                if k == 1:
                    rows = self.rows(half, way)
                    go(self.s1.at[half, way, :, rows], self.r2.at[two, half, way, :, rows], me.near(first, by))
                if k == 3:
                    rows = self.rows(half, way)
                    go(self.s4.at[half, way, rows], self.r4.at[two, half, way, rows], me.near(second, by))
                if k in (2, 4):
                    for sub in self.subs:
                        rows = self.rows(half, sub)
                        if k == 2:
                            go(self.s2.at[half, way, sub, :, rows], self.r3.at[two, half, way, sub, :, rows], me.near(first, by))
                        else:
                            go(self.s5.at[half, way, sub, rows], self.r5.at[two, half, way, sub, rows], me.near(second, by))


def stage_buffers(kind):
    block, last = ((2, NY, NZ, RD, TF), (2, RD, TF)) if kind == "gu" else ((NY, NZ, RF, DC), (RF, DC))
    big, piece, halves = BIG[kind], (40, 128), (2, 2)
    many = (4, *piece)
    vmem, sems = lambda *dims: pltpu.VMEM(dims, BF), pltpu.SemaphoreType.DMA
    return [
        vmem(big, 2, NY, NZ, 2, RD, TF) if kind == "gu" else vmem(big, *block),
        vmem(big, *block),
        vmem(*halves, *many),
        vmem(SMALL, *halves, *many),
        vmem(2, *halves, *many),
        vmem(SMALL, 2, *halves, *many),
        pltpu.VMEM((SMALL, *halves, *many), F32),
        vmem(*halves, *piece),
        vmem(SMALL, *halves, *piece),
        vmem(2, *halves, *piece),
        vmem(SMALL, 2, *halves, *piece),
        vmem(SMALL, NX, *last),
        sems((6, big)),
        sems((6, big)),
    ]


NBUF = 14


def back_kernel(with_da, *refs):
    refs = list(refs)
    take = lambda n: [refs.pop(0) for _ in range(n)]
    a, dy_in, wd, gate, up, dwd = take(6)
    if with_da:
        wgu, h, act = take(3)
        out_gu, out_d, dh, dwd_next = take(4)
    else:
        out_gu, out_d = take(2)
    gu_bufs, d_bufs = take(NBUF), take(NBUF)
    dg_s, du_s, lsem = take(3)
    dy = dy_in
    if with_da:
        da, dy, dsem = take(3)
    i = pl.program_id(0)
    me = Place()
    bring = pltpu.make_async_copy(dy_in, dy, dsem.at[0]) if with_da else None
    save = pltpu.make_async_copy(dy, dh, dsem.at[1]) if with_da else None

    @pl.when(i == 0)
    def _():
        if with_da:
            bring.start()
        me.meet(True)
        if with_da:
            bring.wait()

    own = gu_bufs[0]
    gu = Summing("gu", NT, me, *gu_bufs, out_gu)
    down = Summing("d", NDC, me, *d_bufs, out_d)

    def load(n):
        slot = lax.rem(n, down.big)
        return pltpu.make_async_copy(dwd.at[:, :, me.c, :, cols(n * DC, DC)], down.own.at[slot], lsem.at[slot])

    for k in (6, 5, 4, 3, 2, 1):
        for engine in (gu, down):
            t, there = engine.due(i, k)

            @pl.when(there)
            def _(k=k, engine=engine, t=t):
                if k == 1 and engine is down:
                    load(t).wait()
                engine.compute(k, t)

    for k in (5, 4, 3, 2, 1, 0):
        for engine in (gu, down):
            t, there = engine.due(i, k)

            @pl.when(there)
            def _(k=k, engine=engine, t=t):
                source = None
                if k == 0:
                    source = own.at[lax.rem(t, gu.big), :, :, :, 1 - me.c] if engine is gu else dwd.at[:, :, 1 - me.c, :, cols(t * DC, DC)]
                engine.send(k, t, source)

    @pl.when((i < NDC * down.stride) & (lax.rem(i, down.stride) == 0))
    def _():
        load(lax.div(i, down.stride)).start()

    @pl.when(i < NT)
    def _():
        slot = lax.rem(i, gu.big)
        rows = TOKENS // 4
        for r in range(4):
            part = pl.ds(r * rows, rows)
            dh = dot(dy[part, :], wd[...], 1, 1).astype(BF).astype(F32)
            g, u = gate[part, :], up[part, :]
            sg = jax.nn.sigmoid(g)
            du_s[part, :] = (dh * (g * sg)).astype(BF)
            dg_s[part, :] = (dh * u * (sg * (1 + g * (1 - sg)))).astype(BF)
        own[slot, 0] = dot(a[...], dg_s[...], 0, 0).reshape(NY, NZ, 2, RD, TF).astype(BF)
        own[slot, 1] = dot(a[...], du_s[...], 0, 0).reshape(NY, NZ, 2, RD, TF).astype(BF)
        if with_da:
            more = dot(dg_s[...], wgu[0], 1, 1) + dot(du_s[...], wgu[1], 1, 1)

            @pl.when(i == 0)
            def _():
                da[...] = more

            @pl.when(i > 0)
            def _():
                da[...] += more

    if not with_da:
        return

    @pl.when((i >= NT) & (i < NT + NR))
    def _():
        rows = TOKENS // NR
        part = pl.ds(pl.multiple_of((i - NT) * rows, rows), rows)
        wide, by_a = h[...].astype(F32), da[part, :].astype(BF).astype(F32)
        scale = lax.rsqrt(jnp.mean(wide**2, -1, keepdims=True) + 1e-6)
        by_h = by_a * scale - wide * (scale * scale * scale * jnp.mean(by_a * wide, -1, keepdims=True))
        dy[part, :] = dy[part, :] + by_h.astype(BF)

    @pl.when(i == NT + NR)
    def _():
        save.start()

    tiles = (dg_s, du_s)

    def bring_act(t, slot):
        return pltpu.make_async_copy(act.at[:, cols(t * TF, TF)], tiles[slot], dsem.at[2 + slot])

    @pl.when(i == NT + NR - 1)
    def _():
        bring_act(0, 0).start()

    t = i - NT - NR
    for slot in (0, 1):

        @pl.when((t >= 0) & (lax.rem(t, 2) == slot))
        def _(slot=slot):
            bring_act(t, slot).wait()

            @pl.when(t < NT - 1)
            def _():
                bring_act(t + 1, 1 - slot).start()

            dwd_next[...] = dot(tiles[slot][...], dy[...], 0, 0).astype(BF)

    @pl.when(i == pl.num_programs(0) - 1)
    def _():
        save.wait()


def backward(a, dy, g_d, gate, up, dwd, more, number):
    with_da = more is not None
    vmem, hbm = pl.BlockSpec(memory_space=pltpu.VMEM), pl.BlockSpec(memory_space=pl.ANY)
    shape, sems = jax.ShapeDtypeStruct, pltpu.SemaphoreType.DMA
    tile = pl.BlockSpec((TOKENS, TF), lambda i: (0, upto(i, NT - 1)))
    in_specs = [vmem, hbm if with_da else vmem, pl.BlockSpec((TF, D), lambda i: (upto(i, NT - 1), 0)), tile, tile, hbm]
    out_specs, out_shape = [vmem, vmem], [shape((2, RD, FF), BF), shape((RF, D), BF)]
    scratch = []
    if with_da:
        late = lambda i: above(i - NT - NR)
        in_specs += [
            pl.BlockSpec((2, D, TF), lambda i: (0, 0, upto(i, NT - 1))),
            pl.BlockSpec((TOKENS // NR, D), lambda i: (upto(above(i - NT), NR - 1), 0)),
            hbm,
        ]
        out_specs += [hbm, pl.BlockSpec((TF, D), lambda i: (late(i), 0))]
        out_shape += [shape((TOKENS, D), BF), shape((FF, D), BF)]
        scratch = [pltpu.VMEM((TOKENS, D), F32), pltpu.VMEM((TOKENS, D), BF), sems((4,))]
    return pl.pallas_call(
        functools.partial(back_kernel, with_da),
        grid=(2 * NT + NR if with_da else NT + STAGES,),
        in_specs=in_specs,
        out_specs=out_specs,
        out_shape=out_shape,
        scratch_shapes=[
            *stage_buffers("gu"),
            *stage_buffers("d"),
            pltpu.VMEM((TOKENS, TF), BF),
            pltpu.VMEM((TOKENS, TF), BF),
            sems((BIG["d"],)),
            *scratch,
        ],
        compiler_params=pltpu.CompilerParams(
            collective_id=number, has_side_effects=True, vmem_limit_bytes=VMEM_LIMIT, dimension_semantics=("arbitrary",)
        ),
        cost_estimate=pl.CostEstimate(
            flops=(12 if with_da else 6) * TOKENS * D * FF, bytes_accessed=200_000_000, transcendentals=TOKENS * FF
        ),
        name=f"backward_{number}",
    )(a, dy, g_d, gate, up, dwd.reshape(NY, NZ, 2, RF, D), *(more or ()))


def total_kernel(part, out, b0, b1, b2, ssem, rsem):
    me = Place()
    barrier = pltpu.get_barrier_semaphore()
    rings = [[me.near(axis, by) for by in (1, 2, 3)] for axis in (0, 1)] + [[me.partner()]]
    peers = [peer for ring in rings for peer in ring]
    for peer in peers:
        pl.semaphore_signal(barrier, inc=1, device_id=peer, device_id_type=MESH)
    pl.semaphore_wait(barrier, len(peers))
    value = part[...]
    for k, (buf, place, ring) in enumerate(zip((b0, b1, b2), (me.y, me.z, me.c), rings, strict=True)):
        buf[place] = value
        for peer in ring:
            pltpu.make_async_remote_copy(
                src_ref=buf.at[place], dst_ref=buf.at[place], send_sem=ssem.at[k], recv_sem=rsem.at[k], device_id=peer, device_id_type=MESH
            ).start()
        wait_bytes(buf.at[pl.ds(0, len(ring))], rsem.at[k])
        wait_bytes(buf.at[pl.ds(0, len(ring))], ssem.at[k])
        value = buf[0]
        for n in range(1, len(ring) + 1):
            value = value + buf[n]
    out[...] = value


def over_group(number, collective):
    part = jnp.full((8, 128), number, F32)
    vmem = pl.BlockSpec(memory_space=pltpu.VMEM)
    out = pl.pallas_call(
        total_kernel,
        in_specs=[vmem],
        out_specs=vmem,
        out_shape=jax.ShapeDtypeStruct((8, 128), F32),
        scratch_shapes=[
            pltpu.VMEM((NY, 8, 128), F32),
            pltpu.VMEM((NZ, 8, 128), F32),
            pltpu.VMEM((2, 8, 128), F32),
            pltpu.SemaphoreType.DMA((3,)),
            pltpu.SemaphoreType.DMA((3,)),
        ],
        compiler_params=pltpu.CompilerParams(collective_id=collective, has_side_effects=True),
        name="total",
    )(part)
    return out[0, 0]


def normed(h):
    wide = h.astype(F32)
    scale = lax.rsqrt(jnp.mean(wide**2, -1, keepdims=True) + 1e-6)
    return (wide * scale).astype(BF)


def adamw(w, m, v, g):
    m = 0.9 * m + 0.1 * g
    v = 0.95 * v + 0.05 * g * g
    step = m * lax.rsqrt(v + 1e-8) + 0.1 * w
    return (w - 0.02 * step).astype(BF), m, v


def clipped(gradients, sum_of_squares, count):
    factor = jnp.minimum(1.0, 0.5 * lax.rsqrt(sum_of_squares / count + 1e-30))
    return [g * factor for g in gradients]


def solution(mesh):
    def step(x, dy, *arrays):
        weights, m, v = (arrays[i : i + 3] for i in (0, 3, 6))
        shards = lambda layer: (jnp.stack([weights[0][layer], weights[1][layer]]), weights[2][layer])
        h0, dy = x[0], dy[0]
        _, d0, a0, act0, gate0, up0, h1 = gathered(h0, *shards(0), None, 0)
        gu1, d1, a1, gate1, up1, by_d1 = gathered(h1, *shards(1), dy, 1)
        mine_gu1, mine_d1, dh, by_d0 = backward(a1, dy, d1, gate1, up1, by_d1, (gu1, h1, act0), 2)
        mine_gu0, mine_d0 = backward(a0, dh, d0, gate0, up0, by_d0, None, 3)
        gradients = [jnp.stack([mine_gu0[n], mine_gu1[n]]).astype(F32) for n in (0, 1)] + [jnp.stack([mine_d0, mine_d1]).astype(F32)]
        squares = over_group(sum(jnp.sum(g * g) for g in gradients), 4)
        gradients = clipped(gradients, squares, S * sum(g.size for g in gradients))
        new = [adamw(w.astype(F32), m, v, g) for w, m, v, g in zip(weights, m, v, gradients, strict=True)]
        return tuple(one[which] for which in range(3) for one in new)

    states, cut = P(("rep", "r", "s"), None, None), P(None, "s", None)
    return jax.shard_map(
        step,
        mesh=mesh,
        in_specs=(states, states) + (cut,) * 9,
        out_specs=(P("rep", "s", None),) * 9,
        check_vma=False,
    )
```

```python
import functools

import jax
import jax.numpy as jnp
from jax import lax
from jax.experimental import pallas as pl
from jax.experimental.pallas import tpu as pltpu
from jax.sharding import PartitionSpec as P

NAMES = ("w_gate", "w_up", "w_down")
BF, F32 = jnp.bfloat16, jnp.float32
MESH = pl.DeviceIdType.MESH

TOKENS, D, FF = 2048, 1280, 4864
NY = NZ = NX = 4
S = NY * NZ * 2
RD, RF = D // S, FF // S
TF = 256
HALF = TOKENS // 2
NT = FF // TF
ND = D // TF
VMEM_LIMIT = 67_000_000
AXES = ((0, 1), (1, 0))
OTHERS = (1, 2, 3)
WAYS = ((0, 1), (1, 3))


def dot(a, b, ca, cb):
    return lax.dot_general(a, b, (((ca,), (cb,)), ((), ())), preferred_element_type=F32)


def at(*index):
    return index


def above(i):
    return i * ((i + 64) // 64)


def upto(i, last):
    return last - above(last - i)


def cols(start, size):
    return pl.ds(pl.multiple_of(start, 128), size)


class Place:
    def __init__(self):
        s = lax.axis_index("s")
        self.y, self.z, self.c = lax.div(s, NZ * 2), lax.rem(lax.div(s, 2), NZ), lax.rem(s, 2)
        self.x = lax.axis_index("r")
        self.pos = (self.y, self.z)

    def ring(self, axis, by):
        return lax.rem(self.pos[axis] + by, 4)

    def near(self, axis, by):
        y, z = (self.ring(0, by), self.z) if axis == 0 else (self.y, self.ring(1, by))
        return {"s": (y * NZ + z) * 2 + self.c}

    def partner(self):
        return {"s": (self.y * NZ + self.z) * 2 + 1 - self.c}

    def across(self, by):
        return {"r": lax.rem(self.x + by, NX)}

    def meet(self, x_too):
        barrier = pltpu.get_barrier_semaphore()
        peers = [self.near(axis, by) for axis in (0, 1) for by in (1, 3)] + [self.partner()]
        if x_too:
            peers += [self.across(by) for by in OTHERS]
        for peer in peers:
            pl.semaphore_signal(barrier, inc=1, device_id=peer, device_id_type=MESH)
        pl.semaphore_wait(barrier, len(peers))


def wait_bytes(ref, sem):
    pltpu.make_async_copy(ref, ref, sem).wait()


CH = NT + 2
LAG = 2
LEAD = 5 * LAG + 1
EARLY = 6
LEAD_NEXT = LEAD - EARLY
EARLY_AT = NT + 2 * ND - EARLY - 5 * LAG
STAGES = 7
ALONG_X = (-7, -5, -3, -1, 1, 9, 13, NT - 1)
ALONG_X_NEXT = (-4, -2, 0, 2, 4, 12, 16, NT - 1)
WITHIN = (3, 5, 7, 9, None, None, 11, NT - 1)


def gather_kernel(forward, *refs):
    if forward:
        h, wgu, wd, wgu_next, g_gu, g_d, a_out, act, gate, up, h_new, g_next, wt, wdt, act_s, a, ssem, rsem, lsem, osem = refs
        lead, start_at, along_x = LEAD, 0, ALONG_X
    else:
        h, wgu, wd, dy, _, g_gu, g_d, a_out, gate, up, dwd, wt, act_s, a, ssem, rsem, lsem, osem = refs
        lead, start_at, along_x = LEAD_NEXT, EARLY, ALONG_X_NEXT
    step = pl.program_id(0)
    i = step - lead
    me = Place()
    whole = {"gu": (g_gu, wgu), "next": (g_next, wgu_next)} if forward else {"gu": (g_gu, wgu)}
    own = [
        pltpu.make_async_copy(wd.at[:, cols(t * TF, TF)], g_d.at[me.y, me.z, me.c, :, cols(t * TF, TF)], osem.at[n])
        for n, t in enumerate((me.x, ND - 1))
    ]
    if forward:
        own += [pltpu.make_async_copy(src, dst.at[:, me.y, me.z, me.c], osem.at[2 + n]) for n, (dst, src) in enumerate(whole.values())]

    @pl.when(step == 0)
    def _():
        me.meet(True)
        for copy in own:
            copy.start()

    @pl.when(step == 2 * LAG)
    def _():
        for copy in own:
            copy.wait()

    def block(kind, t, half, sub, y, z, c):
        width = TF if half is None else TF // 2
        start = t * TF + (half or 0) * (TF // 2)
        if kind in whole:
            lead = slice(None) if sub is None else sub
            return whole[kind][0].at[lead, y, z, c, :, cols(start, width)]
        rows = {None: slice(None), 0: pl.ds(0, 80), 1: pl.ds(80, RF - 80)}[sub]
        return g_d.at[y, z, c, rows, cols(start, width)]

    def mine(kind, t, half):
        start = t * TF + half * (TF // 2)
        return whole[kind][1].at[:, :, cols(start, TF // 2)] if kind in whole else wd.at[:, cols(start, TF // 2)]

    ALL = slice(None)

    def cores(kind, t, c):
        return g_d.at[:, :, c, :, 0 : NX * TF] if kind == "x" else block(kind, t, None, None, ALL, ALL, c)

    def totals(kind, t, k):
        c = me.c
        if k == 6:
            return cores(kind, t, c)
        y, z, c = [(pl.ds(0, 2), 0, c), (pl.ds(0, 1), 0, c), (ALL, pl.ds(0, 2), c), (ALL, pl.ds(0, 1), c), (ALL, ALL, ALL), (ALL, ALL, c)][k]
        return block(kind, t, None, None, y, z, c)

    def send(kind, t, ch, k):
        def go(src, dst, peer):
            pltpu.make_async_remote_copy(
                src_ref=src, dst_ref=dst, send_sem=ssem.at[k, ch], recv_sem=rsem.at[k, ch], device_id=peer, device_id_type=MESH
            ).start()

        y, z, c = me.y, me.z, me.c
        if k < 4:
            for half in (0, 1):
                first, second = AXES[half]
                if k == 0:
                    for by in (1, 3):
                        go(mine(kind, t, half), block(kind, t, half, None, y, z, c), me.near(first, by))
                if k == 1:
                    for sub, by in WAYS:
                        back = me.ring(first, 4 - by)
                        ref = block(kind, t, half, sub, *((back, z) if first == 0 else (y, back)), c)
                        go(ref, ref, me.near(first, by))
                if k == 2:
                    ref = block(kind, t, half, None, *((ALL, z) if first == 0 else (y, ALL)), c)
                    for by in (1, 3):
                        go(ref, ref, me.near(second, by))
                if k == 3:
                    for sub, by in WAYS:
                        back = me.ring(second, 4 - by)
                        ref = block(kind, t, half, sub, *((ALL, back) if second == 1 else (back, ALL)), c)
                        go(ref, ref, me.near(second, by))
        if k == 4:
            ref = block(kind, t, None, None, ALL, ALL, c)
            for by in (1, 3):
                go(ref, ref, me.across(by))
        if k == 5:
            for sub, by in WAYS:
                ref = block(kind, lax.rem(me.x + 4 - by, NX), None, sub, ALL, ALL, c)
                go(ref, ref, me.across(by))
        if k == 6:
            ref = cores(kind, t, c)
            go(ref, ref, me.partner())

    def load(kind, t):
        slot = lax.rem(t, 2)
        if kind == "gu":
            return pltpu.make_async_copy(g_gu.at[:, :, :, :, :, cols(t * TF, TF)], wt.at[slot], lsem.at[0, slot])
        return pltpu.make_async_copy(g_d.at[:, :, :, :, cols(t * TF, TF)], wdt.at[slot], lsem.at[1, slot])

    PLANE = (0, 1, 2, 3, 6)

    save = pltpu.make_async_copy(a, a_out, osem.at[4])

    @pl.when(step == 1)
    def _():
        rows = TOKENS // 4
        for r in range(4):
            part = pl.ds(r * rows, rows)
            a[part, :] = normed(h[part, :])

    @pl.when(step == 2)
    def _():
        save.start()

    for n in reversed(range(6)):
        t = i + 1 + (5 - n) * LAG

        @pl.when((t >= start_at) & (t < NT))
        def _(n=n, t=t):
            if n > 0:
                wait_bytes(totals("gu", t, PLANE[n - 1]), rsem.at[PLANE[n - 1], t])
            if n < 5:
                send("gu", t, t, PLANE[n])

        if n == 5:

            @pl.when((t >= 0) & (t < NT))
            def _(t=t):
                load("gu", t).start()

    if forward:
        for n in reversed(range(6)):
            t = i - EARLY_AT - n * LAG

            @pl.when((t >= 0) & (t < EARLY))
            def _(n=n, t=t):
                if n > 0:
                    wait_bytes(totals("next", t, PLANE[n - 1]), rsem.at[PLANE[n - 1], CH + t])
                if n < 5:
                    send("next", t, CH + t, PLANE[n])

    late = (("x", me.x, NT, along_x), ("d", ND - 1, NT + 1, WITHIN))
    for kind, t, ch, due in late:
        stages = [k for k in range(STAGES + 1) if due[k] is not None]
        for before, k in zip([None, *stages], stages):

            @pl.when(i == due[k])
            def _(kind=kind, t=t, ch=ch, before=before, k=k):
                if before is not None:
                    wait_bytes(totals(kind, t, before), rsem.at[before, ch])
                if k < STAGES:
                    send(kind, t, ch, k)

    if forward:

        j = i - NT
        column, lower = lax.div(j, 2), lax.rem(j, 2)

        @pl.when(i == NT - 1)
        def _():
            load("d", 0).start()

        @pl.when((j >= 0) & (lower == 0) & (column < ND - 1))
        def _():
            load("d", column + 1).start()

    @pl.when((i >= 0) & (i < NT))
    def _():
        load("gu", i).wait()
        slot = lax.rem(i, 2)
        g = dot(a[...], wt[slot, 0].reshape(D, TF), 1, 0)
        u = dot(a[...], wt[slot, 1].reshape(D, TF), 1, 0)
        gate[...] = g
        up[...] = u
        hidden = (g * jax.nn.sigmoid(g) * u).astype(BF)
        if forward:
            act[...] = hidden
            act_s[:, cols(i * TF, TF)] = hidden
        else:
            act_s[...] = hidden
            dwd[...] = dot(act_s[...], dy[...], 0, 0).astype(BF)

    if forward:

        @pl.when((j >= 0) & (lower == 0))
        def _():
            load("d", column).wait()

        @pl.when(j >= 0)
        def _():
            part = pl.ds(pl.multiple_of(lower * HALF, HALF), HALF)
            new = dot(act_s[part, :], wdt[lax.rem(column, 2)].reshape(FF, TF), 1, 0).astype(BF)
            h_new[...] = h[part, cols(column * TF, TF)] + new

    @pl.when(step == pl.num_programs(0) - 1)
    def _():
        save.wait()
        for k in PLANE:

            @pl.loop(start_at, NT)
            def _(t, k=k):
                wait_bytes(totals("gu", t, k), ssem.at[k, t])

            if forward:

                @pl.loop(0, EARLY)
                def _(t, k=k):
                    wait_bytes(totals("next", t, k), ssem.at[k, CH + t])

        for kind, t, ch, due in late:
            for k in range(STAGES):
                if due[k] is not None:
                    wait_bytes(totals(kind, t, k), ssem.at[k, ch])


def gathered(h, wgu, wd, other, number):
    forward = number == 0
    lead = LEAD if forward else LEAD_NEXT
    vmem, hbm = pl.BlockSpec(memory_space=pltpu.VMEM), pl.BlockSpec(memory_space=pl.ANY)
    tile = pl.BlockSpec((TOKENS, TF), lambda step: (0, upto(above(step - lead), NT - 1)))
    column = pl.BlockSpec((HALF, TF), lambda step: (above(step - lead - NT) % 2, above(step - lead - NT) // 2))
    row = pl.BlockSpec((TF, D), lambda step: (upto(above(step - lead), NT - 1), 0))
    shape, sems = jax.ShapeDtypeStruct, pltpu.SemaphoreType.DMA
    states, matrices = shape((TOKENS, D), BF), shape((2, NY, NZ, 2, RD, FF), BF)
    wide = [shape((TOKENS, FF), F32)] * 2
    return pl.pallas_call(
        functools.partial(gather_kernel, forward),
        grid=(lead + NT + (2 * ND if forward else 0),),
        in_specs=[vmem, vmem, vmem, vmem, *([] if forward else [hbm])],
        out_specs=[hbm, hbm, hbm, *([tile, tile, tile, column, hbm] if forward else [tile, tile, row])],
        out_shape=[
            matrices,
            shape((NY, NZ, 2, RF, D), BF),
            states,
            *([shape((TOKENS, FF), BF), *wide, states, matrices] if forward else [*wide, shape((FF, D), BF)]),
        ],
        scratch_shapes=[
            pltpu.VMEM((2, 2, NY, NZ, 2, RD, TF), BF),
            *([pltpu.VMEM((2, NY, NZ, 2, RF, TF), BF), pltpu.VMEM((TOKENS, FF), BF)] if forward else [pltpu.VMEM((TOKENS, TF), BF)]),
            pltpu.VMEM((TOKENS, D), BF),
            sems((STAGES, CH + EARLY)),
            sems((STAGES, CH + EARLY)),
            sems((2, 2)),
            sems((5,)),
        ],
        input_output_aliases={} if forward else {4: 0},
        compiler_params=pltpu.CompilerParams(
            collective_id=number, has_side_effects=True, vmem_limit_bytes=VMEM_LIMIT, dimension_semantics=("arbitrary",)
        ),
        name=f"gather_{number}",
    )(h, wgu, wd, *other)


DC = 128
STRIDE = {"gu": 1, "d": 2}
BIG, SMALL = {"gu": 4, "d": 2}, 2
NR = 8
NDC = D // DC


class Summing:
    HEIGHTS = {"gu": ((RD, RD), (RD, RD)), "d": ((40, 40), (40, RF - 120))}

    def __init__(self, kind, count, me, own, inbox, s1, r2, s2, r3, acc, s4, r4, s5, r5, xb, ssem, rsem, out):
        self.kind, self.count, self.me = kind, count, me
        self.stride, self.big = STRIDE[kind], BIG[kind]
        self.own, self.inbox, self.s1, self.r2, self.s2, self.r3 = own, inbox, s1, r2, s2, r3
        self.acc, self.s4, self.r4, self.s5, self.r5, self.xb = acc, s4, r4, s5, r5, xb
        self.ssem, self.rsem, self.out = ssem, rsem, out
        self.subs = (slice(None),) if kind == "gu" else (0, 1)

    def due(self, i, k):
        passed = i - 1 - k
        t = lax.div(passed, self.stride)
        return t, (passed >= 0) & (t < self.count) & (lax.rem(passed, self.stride) == 0)

    def part(self, half, sub):
        if self.kind == "gu":
            return sub, slice(None), pl.ds(half * 128, 128)
        low = 80 * half + 40 * sub
        return 0, pl.ds(low, self.HEIGHTS["d"][half][sub]), slice(None)

    def rows(self, half, sub):
        return slice(None) if self.kind == "gu" else pl.ds(0, self.HEIGHTS["d"][half][sub])

    def both(self, slot, y, z, half, sub):
        lead, rows, columns = self.part(half, sub)
        mine = self.own[slot, lead, y, z, self.me.c, rows, columns] if self.kind == "gu" else self.own[slot, y, z, rows, columns]
        theirs = self.inbox[slot, lead, y, z, rows, columns] if self.kind == "gu" else self.inbox[slot, y, z, rows, columns]
        return mine.astype(F32) + theirs.astype(F32)

    def size(self, k, slot, two):
        if k == 0:
            return self.inbox.at[slot]
        if k == 5:
            return self.xb.at[two, pl.ds(0, 3)]
        if self.kind == "gu":
            return (self.r2, self.r3, self.r4, self.r5)[k - 1].at[two]
        return self.inbox.at[(slot, *((0,), (pl.ds(0, 2),), (0, 0), (0, pl.ds(0, 2)))[k - 1])]

    def compute(self, k, t):
        me, slot, two = self.me, lax.rem(t, self.big), lax.rem(t, SMALL)
        if k > 0:
            wait_bytes(self.size(k - 1, slot, two), self.rsem.at[k - 1, slot])
            wait_bytes(self.size(k - 1, slot, two), self.ssem.at[k - 1, slot])
        if k == 6:
            total = self.xb[two, 0].astype(F32)
            for x in range(1, NX):
                total = total + self.xb[two, x].astype(F32)
            if self.kind == "gu":
                self.out[:, :, cols(t * TF, TF)] = total.astype(BF)
            else:
                self.out[:, cols(t * DC, DC)] = total.astype(BF)
            return
        for half in (0, 1):
            first, second = AXES[half]
            along = lambda place: (place, slice(None)) if first == 0 else (slice(None), place)
            for sub in (0, 1):
                rows = self.rows(half, sub)
                if k == 1:
                    self.s1[half, sub, :, rows] = self.both(slot, *along(me.ring(first, 2)), half, sub).astype(BF)
                if k == 2:
                    for way, by in WAYS:
                        term = self.both(slot, *along(me.ring(first, by)), half, sub)
                        if sub == way:
                            term = term + self.r2[two, half, sub, :, rows].astype(F32)
                        self.s2[half, way, sub, :, rows] = term.astype(BF)
                if k == 3:
                    term = self.both(slot, *along(me.pos[first]), half, sub)
                    for way in (0, 1):
                        term = term + self.r3[two, half, way, sub, :, rows].astype(F32)
                    self.acc[two, half, sub, :, rows] = term
                    self.s4[half, sub, rows] = self.acc[two, half, sub, me.ring(second, 2), rows].astype(BF)
                if k == 4:
                    for way, by in WAYS:
                        term = self.acc[two, half, sub, me.ring(second, by), rows]
                        if sub == way:
                            term = term + self.r4[two, half, sub, rows].astype(F32)
                        self.s5[half, way, sub, rows] = term.astype(BF)
                if k == 5:
                    term = self.acc[two, half, sub, me.pos[second], rows]
                    for way in (0, 1):
                        term = term + self.r5[two, half, way, sub, rows].astype(F32)
                    lead, where, columns = self.part(half, sub)
                    if self.kind == "gu":
                        self.xb[two, me.x, lead, where, columns] = term.astype(BF)
                    else:
                        self.xb[two, me.x, where, columns] = term.astype(BF)

    def send(self, k, t, source=None):
        me, slot, two = self.me, lax.rem(t, self.big), lax.rem(t, SMALL)

        def go(src, dst, peer):
            pltpu.make_async_remote_copy(
                src_ref=src, dst_ref=dst, send_sem=self.ssem.at[k, slot], recv_sem=self.rsem.at[k, slot], device_id=peer, device_id_type=MESH
            ).start()

        if k == 0:
            go(source, self.inbox.at[slot], me.partner())
        if k == 5:
            for by in OTHERS:
                go(self.xb.at[two, me.x], self.xb.at[two, me.x], me.across(by))
        for half in (0, 1):
            first, second = AXES[half]
            for way, by in WAYS:
                if k == 1:
                    rows = self.rows(half, way)
                    go(self.s1.at[half, way, :, rows], self.r2.at[two, half, way, :, rows], me.near(first, by))
                if k == 3:
                    rows = self.rows(half, way)
                    go(self.s4.at[half, way, rows], self.r4.at[two, half, way, rows], me.near(second, by))
                if k in (2, 4):
                    for sub in self.subs:
                        rows = self.rows(half, sub)
                        if k == 2:
                            go(self.s2.at[half, way, sub, :, rows], self.r3.at[two, half, way, sub, :, rows], me.near(first, by))
                        else:
                            go(self.s5.at[half, way, sub, rows], self.r5.at[two, half, way, sub, rows], me.near(second, by))


def stage_buffers(kind):
    block, last = ((2, NY, NZ, RD, TF), (2, RD, TF)) if kind == "gu" else ((NY, NZ, RF, DC), (RF, DC))
    big, piece, halves = BIG[kind], (40, 128), (2, 2)
    many = (4, *piece)
    vmem, sems = lambda *dims: pltpu.VMEM(dims, BF), pltpu.SemaphoreType.DMA
    return [
        vmem(big, 2, NY, NZ, 2, RD, TF) if kind == "gu" else vmem(big, *block),
        vmem(big, *block),
        vmem(*halves, *many),
        vmem(SMALL, *halves, *many),
        vmem(2, *halves, *many),
        vmem(SMALL, 2, *halves, *many),
        pltpu.VMEM((SMALL, *halves, *many), F32),
        vmem(*halves, *piece),
        vmem(SMALL, *halves, *piece),
        vmem(2, *halves, *piece),
        vmem(SMALL, 2, *halves, *piece),
        vmem(SMALL, NX, *last),
        sems((6, big)),
        sems((6, big)),
    ]


NBUF = 14


def back_kernel(with_da, *refs):
    refs = list(refs)
    take = lambda n: [refs.pop(0) for _ in range(n)]
    a, dy_in, wd, gate, up, dwd = take(6)
    if with_da:
        wgu, h, act = take(3)
        out_gu, out_d, dh, dwd_next = take(4)
    else:
        out_gu, out_d = take(2)
    gu_bufs, d_bufs = take(NBUF), take(NBUF)
    dg_s, du_s, lsem = take(3)
    dy = dy_in
    if with_da:
        da, dy, dsem = take(3)
    i = pl.program_id(0)
    me = Place()
    bring = pltpu.make_async_copy(dy_in, dy, dsem.at[0]) if with_da else None
    save = pltpu.make_async_copy(dy, dh, dsem.at[1]) if with_da else None

    @pl.when(i == 0)
    def _():
        if with_da:
            bring.start()
        me.meet(True)
        if with_da:
            bring.wait()

    own = gu_bufs[0]
    gu = Summing("gu", NT, me, *gu_bufs, out_gu)
    down = Summing("d", NDC, me, *d_bufs, out_d)

    def load(n):
        slot = lax.rem(n, down.big)
        return pltpu.make_async_copy(dwd.at[:, :, me.c, :, cols(n * DC, DC)], down.own.at[slot], lsem.at[slot])

    for k in range(6, 0, -1):
        for engine in (gu, down):
            t, there = engine.due(i, k)

            @pl.when(there)
            def _(k=k, engine=engine, t=t):
                if k == 1 and engine is down:
                    load(t).wait()
                engine.compute(k, t)

    for k in reversed(range(6)):
        for engine in (gu, down):
            t, there = engine.due(i, k)

            @pl.when(there)
            def _(k=k, engine=engine, t=t):
                source = None
                if k == 0:
                    source = own.at[lax.rem(t, gu.big), :, :, :, 1 - me.c] if engine is gu else dwd.at[:, :, 1 - me.c, :, cols(t * DC, DC)]
                engine.send(k, t, source)

    @pl.when((i < NDC * down.stride) & (lax.rem(i, down.stride) == 0))
    def _():
        load(lax.div(i, down.stride)).start()

    @pl.when(i < NT)
    def _():
        slot = lax.rem(i, gu.big)
        rows = TOKENS // 4
        for r in range(4):
            part = pl.ds(r * rows, rows)
            dh = dot(dy[part, :], wd[...], 1, 1).astype(BF).astype(F32)
            g, u = gate[part, :], up[part, :]
            sg = jax.nn.sigmoid(g)
            du_s[part, :] = (dh * (g * sg)).astype(BF)
            dg_s[part, :] = (dh * u * (sg * (1 + g * (1 - sg)))).astype(BF)
        own[slot, 0] = dot(a[...], dg_s[...], 0, 0).reshape(NY, NZ, 2, RD, TF).astype(BF)
        own[slot, 1] = dot(a[...], du_s[...], 0, 0).reshape(NY, NZ, 2, RD, TF).astype(BF)
        if with_da:
            more = dot(dg_s[...], wgu[0], 1, 1) + dot(du_s[...], wgu[1], 1, 1)

            @pl.when(i == 0)
            def _():
                da[...] = more

            @pl.when(i > 0)
            def _():
                da[...] += more

    if not with_da:
        return

    @pl.when((i >= NT) & (i < NT + NR))
    def _():
        rows = TOKENS // NR
        part = pl.ds(pl.multiple_of((i - NT) * rows, rows), rows)
        wide, by_a = h[...].astype(F32), da[part, :].astype(BF).astype(F32)
        scale = lax.rsqrt(jnp.mean(wide**2, -1, keepdims=True) + 1e-6)
        by_h = by_a * scale - wide * (scale * scale * scale * jnp.mean(by_a * wide, -1, keepdims=True))
        dy[part, :] = dy[part, :] + by_h.astype(BF)

    @pl.when(i == NT + NR)
    def _():
        save.start()

    tiles = (dg_s, du_s)

    def bring_act(t, slot):
        return pltpu.make_async_copy(act.at[:, cols(t * TF, TF)], tiles[slot], dsem.at[2 + slot])

    @pl.when(i == NT + NR - 1)
    def _():
        bring_act(0, 0).start()

    t = i - NT - NR
    for slot in (0, 1):

        @pl.when((t >= 0) & (lax.rem(t, 2) == slot))
        def _(slot=slot):
            bring_act(t, slot).wait()

            @pl.when(t < NT - 1)
            def _():
                bring_act(t + 1, 1 - slot).start()

            dwd_next[...] = dot(tiles[slot][...], dy[...], 0, 0).astype(BF)

    @pl.when(i == pl.num_programs(0) - 1)
    def _():
        save.wait()


def backward(a, dy, g_d, gate, up, dwd, more, number):
    with_da = more is not None
    vmem, hbm = pl.BlockSpec(memory_space=pltpu.VMEM), pl.BlockSpec(memory_space=pl.ANY)
    shape, sems = jax.ShapeDtypeStruct, pltpu.SemaphoreType.DMA
    tile = pl.BlockSpec((TOKENS, TF), lambda i: (0, upto(i, NT - 1)))
    in_specs = [vmem, hbm if with_da else vmem, pl.BlockSpec((TF, D), lambda i: (upto(i, NT - 1), 0)), tile, tile, hbm]
    out_specs, out_shape = [vmem, vmem], [shape((2, RD, FF), BF), shape((RF, D), BF)]
    scratch = []
    if with_da:
        late = lambda i: above(i - NT - NR)
        in_specs += [
            pl.BlockSpec((2, D, TF), lambda i: (0, 0, upto(i, NT - 1))),
            pl.BlockSpec((TOKENS // NR, D), lambda i: (upto(above(i - NT), NR - 1), 0)),
            hbm,
        ]
        out_specs += [hbm, pl.BlockSpec((TF, D), lambda i: (late(i), 0))]
        out_shape += [shape((TOKENS, D), BF), shape((FF, D), BF)]
        scratch = [pltpu.VMEM((TOKENS, D), F32), pltpu.VMEM((TOKENS, D), BF), sems((4,))]
    return pl.pallas_call(
        functools.partial(back_kernel, with_da),
        grid=(2 * NT + NR if with_da else NT + STAGES,),
        in_specs=in_specs,
        out_specs=out_specs,
        out_shape=out_shape,
        scratch_shapes=[
            *stage_buffers("gu"),
            *stage_buffers("d"),
            pltpu.VMEM((TOKENS, TF), BF),
            pltpu.VMEM((TOKENS, TF), BF),
            sems((BIG["d"],)),
            *scratch,
        ],
        compiler_params=pltpu.CompilerParams(
            collective_id=number, has_side_effects=True, vmem_limit_bytes=VMEM_LIMIT, dimension_semantics=("arbitrary",)
        ),
        name=f"backward_{number}",
    )(a, dy, g_d, gate, up, dwd.reshape(NY, NZ, 2, RF, D), *(more or ()))


def total_kernel(part, out, b0, b1, b2, ssem, rsem):
    me = Place()
    barrier = pltpu.get_barrier_semaphore()
    rings = [[me.near(axis, by) for by in OTHERS] for axis in (0, 1)] + [[me.partner()]]
    peers = [peer for ring in rings for peer in ring]
    for peer in peers:
        pl.semaphore_signal(barrier, inc=1, device_id=peer, device_id_type=MESH)
    pl.semaphore_wait(barrier, len(peers))
    value = part[...]
    for k, (buf, place, ring) in enumerate(zip((b0, b1, b2), (me.y, me.z, me.c), rings, strict=True)):
        buf[place] = value
        for peer in ring:
            pltpu.make_async_remote_copy(
                src_ref=buf.at[place], dst_ref=buf.at[place], send_sem=ssem.at[k], recv_sem=rsem.at[k], device_id=peer, device_id_type=MESH
            ).start()
        wait_bytes(buf.at[pl.ds(0, len(ring))], rsem.at[k])
        wait_bytes(buf.at[pl.ds(0, len(ring))], ssem.at[k])
        value = buf[0]
        for n in range(1, len(ring) + 1):
            value = value + buf[n]
    out[...] = value


def over_group(number, collective):
    part = jnp.full((8, 128), number, F32)
    vmem = pl.BlockSpec(memory_space=pltpu.VMEM)
    out = pl.pallas_call(
        total_kernel,
        in_specs=[vmem],
        out_specs=vmem,
        out_shape=jax.ShapeDtypeStruct((8, 128), F32),
        scratch_shapes=[
            pltpu.VMEM((NY, 8, 128), F32),
            pltpu.VMEM((NZ, 8, 128), F32),
            pltpu.VMEM((2, 8, 128), F32),
            pltpu.SemaphoreType.DMA((3,)),
            pltpu.SemaphoreType.DMA((3,)),
        ],
        compiler_params=pltpu.CompilerParams(collective_id=collective, has_side_effects=True),
        name="total",
    )(part)
    return out[0, 0]


def normed(h):
    wide = h.astype(F32)
    scale = lax.rsqrt(jnp.mean(wide**2, -1, keepdims=True) + 1e-6)
    return (wide * scale).astype(BF)


def adamw(w, m, v, g):
    m = 0.9 * m + 0.1 * g
    v = 0.95 * v + 0.05 * g * g
    step = m * lax.rsqrt(v + 1e-8) + 0.1 * w
    return (w - 0.02 * step).astype(BF), m, v


def clipped(gradients, sum_of_squares, count):
    factor = jnp.minimum(1.0, 0.5 * lax.rsqrt(sum_of_squares / count + 1e-30))
    return [g * factor for g in gradients]


def solution(mesh):
    def step(x, dy, *arrays):
        weights, m, v = (arrays[i : i + 3] for i in (0, 3, 6))
        gu = [jnp.stack([weights[0][layer], weights[1][layer]]) for layer in (0, 1)]
        h0, dy = x[0], dy[0]
        _, d0, a0, act0, gate0, up0, h1, first = gathered(h0, gu[0], weights[2][0], [gu[1]], 0)
        gu1, d1, a1, gate1, up1, by_d1 = gathered(h1, gu[1], weights[2][1], [dy, first], 1)
        gu1, d0, d1 = gu1.reshape(2, D, FF), d0.reshape(FF, D), d1.reshape(FF, D)
        mine_gu1, mine_d1, dh, by_d0 = backward(a1, dy, d1, gate1, up1, by_d1, (gu1, h1, act0), 2)
        mine_gu0, mine_d0 = backward(a0, dh, d0, gate0, up0, by_d0, None, 3)
        gradients = [jnp.stack([mine_gu0[n], mine_gu1[n]]).astype(F32) for n in (0, 1)] + [jnp.stack([mine_d0, mine_d1]).astype(F32)]
        squares = over_group(sum(jnp.sum(g * g) for g in gradients), 4)
        gradients = clipped(gradients, squares, S * sum(g.size for g in gradients))
        new = [adamw(w.astype(F32), m, v, g) for w, m, v, g in zip(weights, m, v, gradients, strict=True)]
        return tuple(one[which] for which in range(3) for one in new)

    states, cut = P(("rep", "r", "s"), None, None), P(None, "s", None)
    return jax.shard_map(
        step,
        mesh=mesh,
        in_specs=(states, states) + (cut,) * 9,
        out_specs=(P("rep", "s", None),) * 9,
        check_vma=False,
    )
```

```python
import functools

import jax
import jax.numpy as jnp
from jax import lax
from jax.experimental import pallas as pl
from jax.experimental.pallas import tpu as pltpu
from jax.sharding import PartitionSpec as P

NAMES = ("w_gate", "w_up", "w_down")
BF, F32 = jnp.bfloat16, jnp.float32
MESH = pl.DeviceIdType.MESH

TOKENS, D, FF = 2048, 1280, 4864
NY = NZ = NX = 4
S = NY * NZ * 2
RD, RF = D // S, FF // S
TF = 256
HALF = TOKENS // 2
NT = FF // TF
ND = D // TF
VMEM_LIMIT = 67_000_000
AXES = ((0, 1), (1, 0))
OTHERS = (1, 2, 3)
WAYS = ((0, 1), (1, 3))


def dot(a, b, ca, cb):
    return lax.dot_general(a, b, (((ca,), (cb,)), ((), ())), preferred_element_type=F32)


def at(*index):
    return index


def above(i):
    return i * ((i + 64) // 64)


def upto(i, last):
    return last - above(last - i)


def cols(start, size):
    return pl.ds(pl.multiple_of(start, 128), size)


class Place:
    def __init__(self):
        s = lax.axis_index("s")
        self.y, self.z, self.c = lax.div(s, NZ * 2), lax.rem(lax.div(s, 2), NZ), lax.rem(s, 2)
        self.x = lax.axis_index("r")
        self.pos = (self.y, self.z)

    def ring(self, axis, by):
        return lax.rem(self.pos[axis] + by, 4)

    def near(self, axis, by):
        y, z = (self.ring(0, by), self.z) if axis == 0 else (self.y, self.ring(1, by))
        return {"s": (y * NZ + z) * 2 + self.c}

    def partner(self):
        return {"s": (self.y * NZ + self.z) * 2 + 1 - self.c}

    def across(self, by):
        return {"r": lax.rem(self.x + by, NX)}

    def meet(self, x_too, far_too=False):
        barrier = pltpu.get_barrier_semaphore()
        peers = [self.near(axis, by) for axis in (0, 1) for by in (1, 3)] + [self.partner()]
        if x_too:
            peers += [self.across(by) for by in OTHERS]
        if far_too:
            peers += [self.near(axis, 2) for axis in (0, 1)]
        for peer in peers:
            pl.semaphore_signal(barrier, inc=1, device_id=peer, device_id_type=MESH)
        pl.semaphore_wait(barrier, len(peers))


def wait_bytes(ref, sem):
    pltpu.make_async_copy(ref, ref, sem).wait()


CH = NT + 2
LAG = 2
LEAD = 5 * LAG + 1
EARLY = 6
LEAD_NEXT = LEAD - EARLY
EARLY_AT = NT + 2 * ND - EARLY - 5 * LAG
STAGES = 7
ALONG_X = (-7, -5, -3, -1, 1, 9, 13, NT - 1)
ALONG_X_NEXT = (-4, -2, 0, 2, 4, 12, 16, NT - 1)
WITHIN = (12, 14, 16, 18, None, None, 20, NT + 2 * ND - 4)
WITHIN_NEXT = (3, 5, 7, 9, None, None, 11, NT - 1)


def gather_kernel(forward, *refs):
    if forward:
        h, shards, downs, g_gu, g_d, a_out, act, gate, up, h_new, g_next, wt, wdt, act_s, a, ssem, rsem, lsem, osem = refs
        lead, start_at, along_x, within = LEAD, 0, ALONG_X, WITHIN
        wgu, wd, wgu_next = shards.at[0], downs.at[0], shards.at[1]
    else:
        h, shards, downs, dy, _, g_gu, g_d, a_out, gate, up, dwd, wt, act_s, a, ssem, rsem, lsem, osem = refs
        lead, start_at, along_x, within = LEAD_NEXT, EARLY, ALONG_X_NEXT, WITHIN_NEXT
        wgu, wd = shards.at[1], downs.at[1]
    step = pl.program_id(0)
    i = step - lead
    me = Place()
    whole = {"gu": (g_gu, wgu), "next": (g_next, wgu_next)} if forward else {"gu": (g_gu, wgu)}
    own = [
        pltpu.make_async_copy(wd.at[:, cols(t * TF, TF)], g_d.at[me.y, me.z, me.c, :, cols(t * TF, TF)], osem.at[n])
        for n, t in enumerate((me.x, ND - 1))
    ]
    if forward:
        own += [pltpu.make_async_copy(src, dst.at[:, me.y, me.z, me.c], osem.at[2 + n]) for n, (dst, src) in enumerate(whole.values())]

    @pl.when(step == 0)
    def _():
        me.meet(True)
        for copy in own:
            copy.start()

    @pl.when(step == 2 * LAG)
    def _():
        for copy in own:
            copy.wait()

    def block(kind, t, half, sub, y, z, c):
        width = TF if half is None else TF // 2
        start = t * TF + (half or 0) * (TF // 2)
        if kind in whole:
            lead = slice(None) if sub is None else sub
            return whole[kind][0].at[lead, y, z, c, :, cols(start, width)]
        rows = {None: slice(None), 0: pl.ds(0, 80), 1: pl.ds(80, RF - 80)}[sub]
        return g_d.at[y, z, c, rows, cols(start, width)]

    def mine(kind, t, half):
        start = t * TF + half * (TF // 2)
        return whole[kind][1].at[:, :, cols(start, TF // 2)] if kind in whole else wd.at[:, cols(start, TF // 2)]

    ALL = slice(None)

    def cores(kind, t, c):
        return g_d.at[:, :, c, :, 0 : NX * TF] if kind == "x" else block(kind, t, None, None, ALL, ALL, c)

    def totals(kind, t, k):
        c = me.c
        if k == 6:
            return cores(kind, t, c)
        y, z, c = [(pl.ds(0, 2), 0, c), (pl.ds(0, 1), 0, c), (ALL, pl.ds(0, 2), c), (ALL, pl.ds(0, 1), c), (ALL, ALL, ALL), (ALL, ALL, c)][k]
        return block(kind, t, None, None, y, z, c)

    def send(kind, t, ch, k):
        def go(src, dst, peer):
            pltpu.make_async_remote_copy(
                src_ref=src, dst_ref=dst, send_sem=ssem.at[k, ch], recv_sem=rsem.at[k, ch], device_id=peer, device_id_type=MESH
            ).start()

        y, z, c = me.y, me.z, me.c
        if k < 4:
            for half in (0, 1):
                first, second = AXES[half]
                if k == 0:
                    for by in (1, 3):
                        go(mine(kind, t, half), block(kind, t, half, None, y, z, c), me.near(first, by))
                if k == 1:
                    for sub, by in WAYS:
                        back = me.ring(first, 4 - by)
                        ref = block(kind, t, half, sub, *((back, z) if first == 0 else (y, back)), c)
                        go(ref, ref, me.near(first, by))
                if k == 2:
                    ref = block(kind, t, half, None, *((ALL, z) if first == 0 else (y, ALL)), c)
                    for by in (1, 3):
                        go(ref, ref, me.near(second, by))
                if k == 3:
                    for sub, by in WAYS:
                        back = me.ring(second, 4 - by)
                        ref = block(kind, t, half, sub, *((ALL, back) if second == 1 else (back, ALL)), c)
                        go(ref, ref, me.near(second, by))
        if k == 4:
            ref = block(kind, t, None, None, ALL, ALL, c)
            for by in (1, 3):
                go(ref, ref, me.across(by))
        if k == 5:
            for sub, by in WAYS:
                ref = block(kind, lax.rem(me.x + 4 - by, NX), None, sub, ALL, ALL, c)
                go(ref, ref, me.across(by))
        if k == 6:
            ref = cores(kind, t, c)
            go(ref, ref, me.partner())

    def load(kind, t):
        slot = lax.rem(t, 2)
        if kind == "gu":
            return pltpu.make_async_copy(g_gu.at[:, :, :, :, :, cols(t * TF, TF)], wt.at[slot], lsem.at[0, slot])
        return pltpu.make_async_copy(g_d.at[:, :, :, :, cols(t * TF, TF)], wdt.at[slot], lsem.at[1, slot])

    PLANE = (0, 1, 2, 3, 6)

    save = pltpu.make_async_copy(a, a_out, osem.at[4])

    @pl.when(step == 1)
    def _():
        rows = TOKENS // 4
        for r in range(4):
            part = pl.ds(r * rows, rows)
            a[part, :] = normed(h[part, :])

    @pl.when(step == 2)
    def _():
        save.start()

    for n in reversed(range(6)):
        t = i + 1 + (5 - n) * LAG

        @pl.when((t >= start_at) & (t < NT))
        def _(n=n, t=t):
            if n > 0:
                wait_bytes(totals("gu", t, PLANE[n - 1]), rsem.at[PLANE[n - 1], t])
            if n < 5:
                send("gu", t, t, PLANE[n])

        if n == 5:

            @pl.when((t >= 0) & (t < NT))
            def _(t=t):
                load("gu", t).start()

    if forward:
        for n in reversed(range(6)):
            t = i - EARLY_AT - n * LAG

            @pl.when((t >= 0) & (t < EARLY))
            def _(n=n, t=t):
                if n > 0:
                    wait_bytes(totals("next", t, PLANE[n - 1]), rsem.at[PLANE[n - 1], CH + t])
                if n < 5:
                    send("next", t, CH + t, PLANE[n])

    late = (("x", me.x, NT, along_x), ("d", ND - 1, NT + 1, within))
    for kind, t, ch, due in late:
        stages = [k for k in range(STAGES + 1) if due[k] is not None]
        for before, k in zip([None, *stages], stages):

            @pl.when(i == due[k])
            def _(kind=kind, t=t, ch=ch, before=before, k=k):
                if before is not None:
                    wait_bytes(totals(kind, t, before), rsem.at[before, ch])
                if k < STAGES:
                    send(kind, t, ch, k)

    if forward:

        j = i - NT
        column, lower = lax.div(j, 2), lax.rem(j, 2)

        @pl.when(i == NT - 1)
        def _():
            load("d", 0).start()

        @pl.when((j >= 0) & (lower == 0) & (column < ND - 1))
        def _():
            load("d", column + 1).start()

    @pl.when((i >= 0) & (i < NT))
    def _():
        load("gu", i).wait()
        slot = lax.rem(i, 2)
        g = dot(a[...], wt[slot, 0].reshape(D, TF), 1, 0)
        u = dot(a[...], wt[slot, 1].reshape(D, TF), 1, 0)
        gate[...] = g
        up[...] = u
        hidden = (g * jax.nn.sigmoid(g) * u).astype(BF)
        if forward:
            act[...] = hidden
            act_s[:, cols(i * TF, TF)] = hidden
        else:
            act_s[...] = hidden
            dwd[...] = dot(act_s[...], dy[...], 0, 0).astype(BF)

    if forward:

        @pl.when((j >= 0) & (lower == 0))
        def _():
            load("d", column).wait()

        @pl.when(j >= 0)
        def _():
            part = pl.ds(pl.multiple_of(lower * HALF, HALF), HALF)
            new = dot(act_s[part, :], wdt[lax.rem(column, 2)].reshape(FF, TF), 1, 0).astype(BF)
            h_new[...] = h[part, cols(column * TF, TF)] + new

    @pl.when(step == pl.num_programs(0) - 1)
    def _():
        save.wait()
        for k in PLANE:

            @pl.loop(start_at, NT)
            def _(t, k=k):
                wait_bytes(totals("gu", t, k), ssem.at[k, t])

            if forward:

                @pl.loop(0, EARLY)
                def _(t, k=k):
                    wait_bytes(totals("next", t, k), ssem.at[k, CH + t])

        for kind, t, ch, due in late:
            for k in range(STAGES):
                if due[k] is not None:
                    wait_bytes(totals(kind, t, k), ssem.at[k, ch])


def gathered(h, shards, downs, other, number):
    forward = number == 0
    lead = LEAD if forward else LEAD_NEXT
    vmem, hbm = pl.BlockSpec(memory_space=pltpu.VMEM), pl.BlockSpec(memory_space=pl.ANY)
    tile = pl.BlockSpec((TOKENS, TF), lambda step: (0, upto(above(step - lead), NT - 1)))
    column = pl.BlockSpec((HALF, TF), lambda step: (above(step - lead - NT) % 2, above(step - lead - NT) // 2))
    row = pl.BlockSpec((TF, D), lambda step: (upto(above(step - lead), NT - 1), 0))
    shape, sems = jax.ShapeDtypeStruct, pltpu.SemaphoreType.DMA
    states, matrices = shape((TOKENS, D), BF), shape((2, NY, NZ, 2, RD, FF), BF)
    wide = [shape((TOKENS, FF), F32)] * 2
    return pl.pallas_call(
        functools.partial(gather_kernel, forward),
        grid=(lead + NT + (2 * ND if forward else 0),),
        in_specs=[vmem, vmem, vmem, *([] if forward else [vmem, hbm])],
        out_specs=[hbm, hbm, hbm, *([tile, tile, tile, column, hbm] if forward else [tile, tile, row])],
        out_shape=[
            matrices,
            shape((NY, NZ, 2, RF, D), BF),
            states,
            *([shape((TOKENS, FF), BF), *wide, states, matrices] if forward else [*wide, shape((FF, D), BF)]),
        ],
        scratch_shapes=[
            pltpu.VMEM((2, 2, NY, NZ, 2, RD, TF), BF),
            *([pltpu.VMEM((2, NY, NZ, 2, RF, TF), BF), pltpu.VMEM((TOKENS, FF), BF)] if forward else [pltpu.VMEM((TOKENS, TF), BF)]),
            pltpu.VMEM((TOKENS, D), BF),
            sems((STAGES, CH + EARLY)),
            sems((STAGES, CH + EARLY)),
            sems((2, 2)),
            sems((5,)),
        ],
        input_output_aliases={} if forward else {4: 0},
        compiler_params=pltpu.CompilerParams(
            collective_id=number, has_side_effects=True, vmem_limit_bytes=VMEM_LIMIT, dimension_semantics=("arbitrary",)
        ),
        name=f"gather_{number}",
    )(h, shards, downs, *other)


DC = 128
STRIDE = {"gu": 1, "d": 2}
BIG, SMALL = {"gu": 4, "d": 2}, 2
NR = 8
NDC = D // DC


class Summing:
    HEIGHTS = {"gu": ((RD, RD), (RD, RD)), "d": ((40, 40), (40, RF - 120))}

    def __init__(self, kind, count, me, own, inbox, s1, r2, s2, r3, acc, s4, r4, s5, r5, xb, ssem, rsem, out):
        self.kind, self.count, self.me = kind, count, me
        self.stride, self.big = STRIDE[kind], BIG[kind]
        self.own, self.inbox, self.s1, self.r2, self.s2, self.r3 = own, inbox, s1, r2, s2, r3
        self.acc, self.s4, self.r4, self.s5, self.r5, self.xb = acc, s4, r4, s5, r5, xb
        self.ssem, self.rsem, self.out = ssem, rsem, out
        self.subs = (slice(None),) if kind == "gu" else (0, 1)

    def due(self, i, k):
        passed = i - 1 - k
        t = lax.div(passed, self.stride)
        return t, (passed >= 0) & (t < self.count) & (lax.rem(passed, self.stride) == 0)

    def part(self, half, sub):
        if self.kind == "gu":
            return sub, slice(None), pl.ds(half * 128, 128)
        low = 80 * half + 40 * sub
        return 0, pl.ds(low, self.HEIGHTS["d"][half][sub]), slice(None)

    def rows(self, half, sub):
        return slice(None) if self.kind == "gu" else pl.ds(0, self.HEIGHTS["d"][half][sub])

    def both(self, slot, y, z, half, sub):
        lead, rows, columns = self.part(half, sub)
        mine = self.own[slot, lead, y, z, self.me.c, rows, columns] if self.kind == "gu" else self.own[slot, y, z, rows, columns]
        theirs = self.inbox[slot, lead, y, z, rows, columns] if self.kind == "gu" else self.inbox[slot, y, z, rows, columns]
        return mine.astype(F32) + theirs.astype(F32)

    def size(self, k, slot, two):
        if k == 0:
            return self.inbox.at[slot]
        if k == 5:
            return self.xb.at[two, pl.ds(0, 3)]
        if self.kind == "gu":
            return (self.r2, self.r3, self.r4, self.r5)[k - 1].at[two]
        return self.inbox.at[(slot, *((0,), (pl.ds(0, 2),), (0, 0), (0, pl.ds(0, 2)))[k - 1])]

    def compute(self, k, t):
        me, slot, two = self.me, lax.rem(t, self.big), lax.rem(t, SMALL)
        if k > 0:
            wait_bytes(self.size(k - 1, slot, two), self.rsem.at[k - 1, slot])
            wait_bytes(self.size(k - 1, slot, two), self.ssem.at[k - 1, slot])
        if k == 6:
            total = self.xb[two, 0].astype(F32)
            for x in range(1, NX):
                total = total + self.xb[two, x].astype(F32)
            if self.kind == "gu":
                self.out[:, :, cols(t * TF, TF)] = total.astype(BF)
            else:
                self.out[:, cols(t * DC, DC)] = total.astype(BF)
            return
        for half in (0, 1):
            first, second = AXES[half]
            along = lambda place: (place, slice(None)) if first == 0 else (slice(None), place)
            for sub in (0, 1):
                rows = self.rows(half, sub)
                if k == 1:
                    self.s1[half, sub, :, rows] = self.both(slot, *along(me.ring(first, 2)), half, sub).astype(BF)
                if k == 2:
                    for way, by in WAYS:
                        term = self.both(slot, *along(me.ring(first, by)), half, sub)
                        if sub == way:
                            term = term + self.r2[two, half, sub, :, rows].astype(F32)
                        self.s2[half, way, sub, :, rows] = term.astype(BF)
                if k == 3:
                    term = self.both(slot, *along(me.pos[first]), half, sub)
                    for way in (0, 1):
                        term = term + self.r3[two, half, way, sub, :, rows].astype(F32)
                    self.acc[two, half, sub, :, rows] = term
                    self.s4[half, sub, rows] = self.acc[two, half, sub, me.ring(second, 2), rows].astype(BF)
                if k == 4:
                    for way, by in WAYS:
                        term = self.acc[two, half, sub, me.ring(second, by), rows]
                        if sub == way:
                            term = term + self.r4[two, half, sub, rows].astype(F32)
                        self.s5[half, way, sub, rows] = term.astype(BF)
                if k == 5:
                    term = self.acc[two, half, sub, me.pos[second], rows]
                    for way in (0, 1):
                        term = term + self.r5[two, half, way, sub, rows].astype(F32)
                    lead, where, columns = self.part(half, sub)
                    if self.kind == "gu":
                        self.xb[two, me.x, lead, where, columns] = term.astype(BF)
                    else:
                        self.xb[two, me.x, where, columns] = term.astype(BF)

    def send(self, k, t, source=None):
        me, slot, two = self.me, lax.rem(t, self.big), lax.rem(t, SMALL)

        def go(src, dst, peer):
            pltpu.make_async_remote_copy(
                src_ref=src, dst_ref=dst, send_sem=self.ssem.at[k, slot], recv_sem=self.rsem.at[k, slot], device_id=peer, device_id_type=MESH
            ).start()

        if k == 0:
            go(source, self.inbox.at[slot], me.partner())
        if k == 5:
            for by in OTHERS:
                go(self.xb.at[two, me.x], self.xb.at[two, me.x], me.across(by))
        for half in (0, 1):
            first, second = AXES[half]
            for way, by in WAYS:
                if k == 1:
                    rows = self.rows(half, way)
                    go(self.s1.at[half, way, :, rows], self.r2.at[two, half, way, :, rows], me.near(first, by))
                if k == 3:
                    rows = self.rows(half, way)
                    go(self.s4.at[half, way, rows], self.r4.at[two, half, way, rows], me.near(second, by))
                if k in (2, 4):
                    for sub in self.subs:
                        rows = self.rows(half, sub)
                        if k == 2:
                            go(self.s2.at[half, way, sub, :, rows], self.r3.at[two, half, way, sub, :, rows], me.near(first, by))
                        else:
                            go(self.s5.at[half, way, sub, rows], self.r5.at[two, half, way, sub, rows], me.near(second, by))


def stage_buffers(kind):
    block, last = ((2, NY, NZ, RD, TF), (2, RD, TF)) if kind == "gu" else ((NY, NZ, RF, DC), (RF, DC))
    big, piece, halves = BIG[kind], (40, 128), (2, 2)
    many = (4, *piece)
    vmem, sems = lambda *dims: pltpu.VMEM(dims, BF), pltpu.SemaphoreType.DMA
    return [
        vmem(big, 2, NY, NZ, 2, RD, TF) if kind == "gu" else vmem(big, *block),
        vmem(big, *block),
        vmem(*halves, *many),
        vmem(SMALL, *halves, *many),
        vmem(2, *halves, *many),
        vmem(SMALL, 2, *halves, *many),
        pltpu.VMEM((SMALL, *halves, *many), F32),
        vmem(*halves, *piece),
        vmem(SMALL, *halves, *piece),
        vmem(2, *halves, *piece),
        vmem(SMALL, 2, *halves, *piece),
        vmem(SMALL, NX, *last),
        sems((6, big)),
        sems((6, big)),
    ]


NBUF = 14


def sum_over_group(me, value, out, bufs, ssem, rsem):
    rings = [[me.near(axis, by) for by in OTHERS] for axis in (0, 1)] + [[me.partner()]]
    for k, (buf, place, ring) in enumerate(zip(bufs, (me.y, me.z, me.c), rings)):
        buf[place] = value
        for peer in ring:
            pltpu.make_async_remote_copy(
                src_ref=buf.at[place], dst_ref=buf.at[place], send_sem=ssem.at[k], recv_sem=rsem.at[k], device_id=peer, device_id_type=MESH
            ).start()
        wait_bytes(buf.at[pl.ds(0, len(ring))], rsem.at[k])
        wait_bytes(buf.at[pl.ds(0, len(ring))], ssem.at[k])
        value = buf[0]
        for n in range(1, len(ring) + 1):
            value = value + buf[n]
    out[...] = value


def back_kernel(with_da, *refs):
    refs = list(refs)
    take = lambda n: [refs.pop(0) for _ in range(n)]
    a, dy_in, wd, gate, up, dwd = take(6)
    if with_da:
        wgu, h, act = take(3)
        out_gu, out_d, dh, dwd_next = take(4)
    else:
        parts = take(2)
        out_gu, out_d, total = take(3)
    gu_bufs, d_bufs = take(NBUF), take(NBUF)
    dg_s, du_s, lsem = take(3)
    dy = dy_in
    if with_da:
        da, dy, dsem = take(3)
    else:
        rings = take(3)
        tsems = take(2)
    i = pl.program_id(0)
    me = Place()
    bring = pltpu.make_async_copy(dy_in, dy, dsem.at[0]) if with_da else None
    save = pltpu.make_async_copy(dy, dh, dsem.at[1]) if with_da else None

    @pl.when(i == 0)
    def _():
        if with_da:
            bring.start()
        me.meet(True, not with_da)
        if with_da:
            bring.wait()

    own = gu_bufs[0]
    gu = Summing("gu", NT, me, *gu_bufs, out_gu)
    down = Summing("d", NDC, me, *d_bufs, out_d)

    def load(n):
        slot = lax.rem(n, down.big)
        return pltpu.make_async_copy(dwd.at[:, :, me.c, :, cols(n * DC, DC)], down.own.at[slot], lsem.at[slot])

    for k in range(6, 0, -1):
        for engine in (gu, down):
            t, there = engine.due(i, k)

            @pl.when(there)
            def _(k=k, engine=engine, t=t):
                if k == 1 and engine is down:
                    load(t).wait()
                engine.compute(k, t)

    for k in reversed(range(6)):
        for engine in (gu, down):
            t, there = engine.due(i, k)

            @pl.when(there)
            def _(k=k, engine=engine, t=t):
                source = None
                if k == 0:
                    source = own.at[lax.rem(t, gu.big), :, :, :, 1 - me.c] if engine is gu else dwd.at[:, :, 1 - me.c, :, cols(t * DC, DC)]
                engine.send(k, t, source)

    @pl.when((i < NDC * down.stride) & (lax.rem(i, down.stride) == 0))
    def _():
        load(lax.div(i, down.stride)).start()

    @pl.when(i < NT)
    def _():
        slot = lax.rem(i, gu.big)
        rows = TOKENS // 4
        for r in range(4):
            part = pl.ds(r * rows, rows)
            dh = dot(dy[part, :], wd[...], 1, 1).astype(BF).astype(F32)
            g, u = gate[part, :], up[part, :]
            sg = jax.nn.sigmoid(g)
            du_s[part, :] = (dh * (g * sg)).astype(BF)
            dg_s[part, :] = (dh * u * (sg * (1 + g * (1 - sg)))).astype(BF)
        own[slot, 0] = dot(a[...], dg_s[...], 0, 0).reshape(NY, NZ, 2, RD, TF).astype(BF)
        own[slot, 1] = dot(a[...], du_s[...], 0, 0).reshape(NY, NZ, 2, RD, TF).astype(BF)
        if with_da:
            more = dot(dg_s[...], wgu[0], 1, 1) + dot(du_s[...], wgu[1], 1, 1)

            @pl.when(i == 0)
            def _():
                da[...] = more

            @pl.when(i > 0)
            def _():
                da[...] += more

    if not with_da:

        @pl.when(i == pl.num_programs(0) - 1)
        def _():
            squares = jnp.zeros((8, 128), F32)
            for ref in (*parts, out_gu, out_d):
                for block in (ref,) if len(ref.shape) == 2 else (ref.at[0], ref.at[1]):
                    squares = squares + jnp.sum(block[...].astype(F32) ** 2)
            sum_over_group(me, squares, total, rings, *tsems)

        return

    @pl.when((i >= NT) & (i < NT + NR))
    def _():
        rows = TOKENS // NR
        part = pl.ds(pl.multiple_of((i - NT) * rows, rows), rows)
        wide, by_a = h[...].astype(F32), da[part, :].astype(BF).astype(F32)
        scale = lax.rsqrt(jnp.mean(wide**2, -1, keepdims=True) + 1e-6)
        by_h = by_a * scale - wide * (scale * scale * scale * jnp.mean(by_a * wide, -1, keepdims=True))
        dy[part, :] = dy[part, :] + by_h.astype(BF)

    @pl.when(i == NT + NR)
    def _():
        save.start()

    tiles = (dg_s, du_s)

    def bring_act(t, slot):
        return pltpu.make_async_copy(act.at[:, cols(t * TF, TF)], tiles[slot], dsem.at[2 + slot])

    @pl.when(i == NT + NR - 1)
    def _():
        bring_act(0, 0).start()

    t = i - NT - NR
    for slot in (0, 1):

        @pl.when((t >= 0) & (lax.rem(t, 2) == slot))
        def _(slot=slot):
            bring_act(t, slot).wait()

            @pl.when(t < NT - 1)
            def _():
                bring_act(t + 1, 1 - slot).start()

            dwd_next[...] = dot(tiles[slot][...], dy[...], 0, 0).astype(BF)

    @pl.when(i == pl.num_programs(0) - 1)
    def _():
        save.wait()


def backward(a, dy, g_d, gate, up, dwd, more, number):
    with_da = number == 2
    vmem, hbm = pl.BlockSpec(memory_space=pltpu.VMEM), pl.BlockSpec(memory_space=pl.ANY)
    shape, sems = jax.ShapeDtypeStruct, pltpu.SemaphoreType.DMA
    tile = pl.BlockSpec((TOKENS, TF), lambda i: (0, upto(i, NT - 1)))
    in_specs = [vmem, hbm if with_da else vmem, pl.BlockSpec((TF, D), lambda i: (upto(i, NT - 1), 0)), tile, tile, hbm]
    out_specs, out_shape = [vmem, vmem], [shape((2, RD, FF), BF), shape((RF, D), BF)]
    scratch = []
    if with_da:
        late = lambda i: above(i - NT - NR)
        in_specs += [
            pl.BlockSpec((2, D, TF), lambda i: (0, 0, upto(i, NT - 1))),
            pl.BlockSpec((TOKENS // NR, D), lambda i: (upto(above(i - NT), NR - 1), 0)),
            hbm,
        ]
        out_specs += [hbm, pl.BlockSpec((TF, D), lambda i: (late(i), 0))]
        out_shape += [shape((TOKENS, D), BF), shape((FF, D), BF)]
        scratch = [pltpu.VMEM((TOKENS, D), F32), pltpu.VMEM((TOKENS, D), BF), sems((4,))]
    else:
        tiny = (8, 128)
        in_specs += [vmem, vmem]
        out_specs += [vmem]
        out_shape += [shape(tiny, F32)]
        scratch = [*(pltpu.VMEM((n, *tiny), F32) for n in (NY, NZ, 2)), sems((3,)), sems((3,))]
    return pl.pallas_call(
        functools.partial(back_kernel, with_da),
        grid=(2 * NT + NR if with_da else NT + STAGES,),
        in_specs=in_specs,
        out_specs=out_specs,
        out_shape=out_shape,
        scratch_shapes=[
            *stage_buffers("gu"),
            *stage_buffers("d"),
            pltpu.VMEM((TOKENS, TF), BF),
            pltpu.VMEM((TOKENS, TF), BF),
            sems((BIG["d"],)),
            *scratch,
        ],
        compiler_params=pltpu.CompilerParams(
            collective_id=number, has_side_effects=True, vmem_limit_bytes=VMEM_LIMIT, dimension_semantics=("arbitrary",)
        ),
        name=f"backward_{number}",
    )(a, dy, g_d, gate, up, dwd.reshape(NY, NZ, 2, RF, D), *more)


def normed(h):
    wide = h.astype(F32)
    scale = lax.rsqrt(jnp.mean(wide**2, -1, keepdims=True) + 1e-6)
    return (wide * scale).astype(BF)


def adamw(w, m, v, g):
    m = 0.9 * m + 0.1 * g
    v = 0.95 * v + 0.05 * g * g
    step = m * lax.rsqrt(v + 1e-8) + 0.1 * w
    return (w - 0.02 * step).astype(BF), m, v


def clipped(gradients, sum_of_squares, count):
    factor = jnp.minimum(1.0, 0.5 * lax.rsqrt(sum_of_squares / count + 1e-30))
    return [g * factor for g in gradients]


def solution(mesh):
    def step(x, dy, *arrays):
        weights, m, v = (arrays[i : i + 3] for i in (0, 3, 6))
        shards = jnp.stack(weights[:2], 1), weights[2]
        h0, dy = x[0], dy[0]
        _, d0, a0, act0, gate0, up0, h1, first = gathered(h0, *shards, [], 0)
        gu1, d1, a1, gate1, up1, by_d1 = gathered(h1, *shards, [dy, first], 1)
        gu1, d0, d1 = gu1.reshape(2, D, FF), d0.reshape(FF, D), d1.reshape(FF, D)
        mine_gu1, mine_d1, dh, by_d0 = backward(a1, dy, d1, gate1, up1, by_d1, (gu1, h1, act0), 2)
        mine_gu0, mine_d0, squares = backward(a0, dh, d0, gate0, up0, by_d0, (mine_gu1, mine_d1), 3)
        gradients = [jnp.stack([mine_gu0[n], mine_gu1[n]]).astype(F32) for n in (0, 1)] + [jnp.stack([mine_d0, mine_d1]).astype(F32)]
        gradients = clipped(gradients, squares[0, 0], S * sum(g.size for g in gradients))
        new = [adamw(w.astype(F32), m, v, g) for w, m, v, g in zip(weights, m, v, gradients, strict=True)]
        return tuple(one[which] for which in range(3) for one in new)

    states, cut = P(("rep", "r", "s"), None, None), P(None, "s", None)
    return jax.shard_map(
        step,
        mesh=mesh,
        in_specs=(states, states) + (cut,) * 9,
        out_specs=(P("rep", "s", None),) * 9,
        check_vma=False,
    )
```

```python
import functools

import jax
import jax.numpy as jnp
from jax import lax
from jax.experimental import pallas as pl
from jax.experimental.pallas import tpu as pltpu
from jax.sharding import PartitionSpec as P

NAMES = ("w_gate", "w_up", "w_down")
BF, F32 = jnp.bfloat16, jnp.float32
MESH = pl.DeviceIdType.MESH

TOKENS, D, FF = 2048, 1280, 4864
NY = NZ = NX = 4
S = NY * NZ * 2
RD, RF = D // S, FF // S
TF = 256
HALF = TOKENS // 2
LANES = 128
NT = FF // TF
ND = D // TF
VMEM_LIMIT = 67_000_000
AXES = ((0, 1), (1, 0))
OTHERS = (1, 2, 3)
WAYS = ((0, 1), (1, 3))


def dot(a, b, ca, cb):
    return lax.dot_general(a, b, (((ca,), (cb,)), ((), ())), preferred_element_type=F32)


def at(*index):
    return index


def above(i):
    return i * ((i + 64) // 64)


def upto(i, last):
    return last - above(last - i)


def cols(start, size):
    return pl.ds(pl.multiple_of(start, LANES), size)


class Place:
    def __init__(self):
        s = lax.axis_index("s")
        self.y, self.z, self.c = lax.div(s, NZ * 2), lax.rem(lax.div(s, 2), NZ), lax.rem(s, 2)
        self.x = lax.axis_index("r")
        self.pos = (self.y, self.z)

    def ring(self, axis, by):
        return lax.rem(self.pos[axis] + by, 4)

    def near(self, axis, by):
        y, z = (self.ring(0, by), self.z) if axis == 0 else (self.y, self.ring(1, by))
        return {"s": (y * NZ + z) * 2 + self.c}

    def partner(self):
        return {"s": (self.y * NZ + self.z) * 2 + 1 - self.c}

    def across(self, by):
        return {"r": lax.rem(self.x + by, NX)}

    def meet(self, x_too, far_too=False):
        barrier = pltpu.get_barrier_semaphore()
        peers = [self.near(axis, by) for axis in (0, 1) for by in (1, 3)] + [self.partner()]
        if x_too:
            peers += [self.across(by) for by in OTHERS]
        if far_too:
            peers += [self.near(axis, 2) for axis in (0, 1)]
        for peer in peers:
            pl.semaphore_signal(barrier, inc=1, device_id=peer, device_id_type=MESH)
        pl.semaphore_wait(barrier, len(peers))


def wait_bytes(ref, sem):
    pltpu.make_async_copy(ref, ref, sem).wait()


CH = NT + 2
LAG = 2
LEAD = 5 * LAG + 1
EARLY = 6
LEAD_NEXT = LEAD - EARLY
EARLY_AT = NT + 2 * ND - EARLY - 5 * LAG
STAGES = 7
ALONG_X = (-7, -5, -3, -1, 1, 9, 13, NT - 1)
ALONG_X_NEXT = (-4, -2, 0, 2, 4, 12, 16, NT - 1)
WITHIN = (12, 14, 16, 18, None, None, 20, NT + 2 * ND - 4)
WITHIN_NEXT = (3, 5, 7, 9, None, None, 11, NT - 1)


def gather_kernel(forward, *refs):
    if forward:
        h, shards, downs, g_gu, g_d, a_out, act, gate, up, h_new, g_next, wt, wdt, act_s, a, ssem, rsem, lsem, osem = refs
        lead, start_at, along_x, within = LEAD, 0, ALONG_X, WITHIN
        wgu, wd, wgu_next = shards.at[0], downs.at[0], shards.at[1]
    else:
        h, shards, downs, dy, _, g_gu, g_d, a_out, gate, up, dwd, wt, act_s, a, ssem, rsem, lsem, osem = refs
        lead, start_at, along_x, within = LEAD_NEXT, EARLY, ALONG_X_NEXT, WITHIN_NEXT
        wgu, wd = shards.at[1], downs.at[1]
    step = pl.program_id(0)
    i = step - lead
    me = Place()
    whole = {"gu": (g_gu, wgu), "next": (g_next, wgu_next)} if forward else {"gu": (g_gu, wgu)}
    own = [
        pltpu.make_async_copy(wd.at[:, cols(t * TF, TF)], g_d.at[me.y, me.z, me.c, :, cols(t * TF, TF)], osem.at[n])
        for n, t in enumerate((me.x, ND - 1))
    ]

    def own_tile(t, kind, sem):
        dst, src = whole[kind]
        return pltpu.make_async_copy(src.at[:, :, cols(t * TF, TF)], dst.at[t, :, me.y, me.z, me.c], sem)

    @pl.when(step == 0)
    def _():
        me.meet(True)
        for copy in own:
            copy.start()
        if forward:
            for n, kind in enumerate(whole):
                pl.loop(0, NT)(lambda t, n=n, kind=kind: own_tile(t, kind, osem.at[2 + n]).start())

    @pl.when(step == 2 * LAG)
    def _():
        for copy in own:
            copy.wait()
        if forward:
            for n, (_, src) in enumerate(whole.values()):
                wait_bytes(src, osem.at[2 + n])

    def block(kind, t, half, sub, y, z, c):
        if kind in whole:
            lead, columns = slice(None) if half is None else half, slice(None) if sub is None else cols(sub * LANES, LANES)
            return whole[kind][0].at[t, lead, y, z, c, :, columns]
        width = TF if half is None else TF // 2
        start = t * TF + (half or 0) * (TF // 2)
        rows = {None: slice(None), 0: pl.ds(0, 80), 1: pl.ds(80, RF - 80)}[sub]
        return g_d.at[y, z, c, rows, cols(start, width)]

    def mine(kind, t, half):
        return whole[kind][1].at[half, :, cols(t * TF, TF)] if kind in whole else wd.at[:, cols(t * TF + half * LANES, LANES)]

    ALL = slice(None)

    def cores(kind, t, c):
        return g_d.at[:, :, c, :, 0 : NX * TF] if kind == "x" else block(kind, t, None, None, ALL, ALL, c)

    def totals(kind, t, k):
        c = me.c
        if k == 6:
            return cores(kind, t, c)
        y, z, c = [(pl.ds(0, 2), 0, c), (pl.ds(0, 1), 0, c), (ALL, pl.ds(0, 2), c), (ALL, pl.ds(0, 1), c), (ALL, ALL, ALL), (ALL, ALL, c)][k]
        return block(kind, t, None, None, y, z, c)

    def send(kind, t, ch, k):
        def go(src, dst, peer):
            pltpu.make_async_remote_copy(
                src_ref=src, dst_ref=dst, send_sem=ssem.at[k, ch], recv_sem=rsem.at[k, ch], device_id=peer, device_id_type=MESH
            ).start()

        y, z, c = me.y, me.z, me.c
        if k < 4:
            for half in (0, 1):
                first, second = AXES[half]
                if k == 0:
                    for by in (1, 3):
                        go(mine(kind, t, half), block(kind, t, half, None, y, z, c), me.near(first, by))
                if k == 1:
                    for sub, by in WAYS:
                        back = me.ring(first, 4 - by)
                        ref = block(kind, t, half, sub, *((back, z) if first == 0 else (y, back)), c)
                        go(ref, ref, me.near(first, by))
                if k == 2:
                    ref = block(kind, t, half, None, *((ALL, z) if first == 0 else (y, ALL)), c)
                    for by in (1, 3):
                        go(ref, ref, me.near(second, by))
                if k == 3:
                    for sub, by in WAYS:
                        back = me.ring(second, 4 - by)
                        ref = block(kind, t, half, sub, *((ALL, back) if second == 1 else (back, ALL)), c)
                        go(ref, ref, me.near(second, by))
        if k == 4:
            ref = block(kind, t, None, None, ALL, ALL, c)
            for by in (1, 3):
                go(ref, ref, me.across(by))
        if k == 5:
            for sub, by in WAYS:
                ref = block(kind, lax.rem(me.x + 4 - by, NX), None, sub, ALL, ALL, c)
                go(ref, ref, me.across(by))
        if k == 6:
            ref = cores(kind, t, c)
            go(ref, ref, me.partner())

    def load(kind, t):
        slot = lax.rem(t, 2)
        if kind == "gu":
            return pltpu.make_async_copy(g_gu.at[t], wt.at[slot], lsem.at[0, slot])
        return pltpu.make_async_copy(g_d.at[:, :, :, :, cols(t * TF, TF)], wdt.at[slot], lsem.at[1, slot])

    PLANE = (0, 1, 2, 3, 6)

    save = pltpu.make_async_copy(a, a_out, osem.at[4])

    @pl.when(step == 1)
    def _():
        rows = TOKENS // 4
        for r in range(4):
            part = pl.ds(r * rows, rows)
            a[part, :] = normed(h[part, :])

    @pl.when(step == 2)
    def _():
        save.start()

    for n in reversed(range(6)):
        t = i + 1 + (5 - n) * LAG

        @pl.when((t >= start_at) & (t < NT))
        def _(n=n, t=t):
            if n > 0:
                wait_bytes(totals("gu", t, PLANE[n - 1]), rsem.at[PLANE[n - 1], t])
            if n < 5:
                send("gu", t, t, PLANE[n])

        if n == 5:

            @pl.when((t >= 0) & (t < NT))
            def _(t=t):
                load("gu", t).start()

    if forward:
        for n in reversed(range(6)):
            t = i - EARLY_AT - n * LAG

            @pl.when((t >= 0) & (t < EARLY))
            def _(n=n, t=t):
                if n > 0:
                    wait_bytes(totals("next", t, PLANE[n - 1]), rsem.at[PLANE[n - 1], CH + t])
                if n < 5:
                    send("next", t, CH + t, PLANE[n])

    late = (("x", me.x, NT, along_x), ("d", ND - 1, NT + 1, within))
    for kind, t, ch, due in late:
        stages = [k for k in range(STAGES + 1) if due[k] is not None]
        for before, k in zip([None, *stages], stages):

            @pl.when(i == due[k])
            def _(kind=kind, t=t, ch=ch, before=before, k=k):
                if before is not None:
                    wait_bytes(totals(kind, t, before), rsem.at[before, ch])
                if k < STAGES:
                    send(kind, t, ch, k)

    if forward:

        j = i - NT
        column, lower = lax.div(j, 2), lax.rem(j, 2)

        @pl.when(i == NT - 1)
        def _():
            load("d", 0).start()

        @pl.when((j >= 0) & (lower == 0) & (column < ND - 1))
        def _():
            load("d", column + 1).start()

    @pl.when((i >= 0) & (i < NT))
    def _():
        load("gu", i).wait()
        slot = lax.rem(i, 2)
        g = dot(a[...], wt[slot, 0].reshape(D, TF), 1, 0)
        u = dot(a[...], wt[slot, 1].reshape(D, TF), 1, 0)
        gate[...] = g
        up[...] = u
        hidden = (g * jax.nn.sigmoid(g) * u).astype(BF)
        if forward:
            act[...] = hidden
            act_s[:, cols(i * TF, TF)] = hidden
        else:
            act_s[...] = hidden
            dwd[...] = dot(act_s[...], dy[...], 0, 0).astype(BF)

    if forward:

        @pl.when((j >= 0) & (lower == 0))
        def _():
            load("d", column).wait()

        @pl.when(j >= 0)
        def _():
            part = pl.ds(pl.multiple_of(lower * HALF, HALF), HALF)
            new = dot(act_s[part, :], wdt[lax.rem(column, 2)].reshape(FF, TF), 1, 0).astype(BF)
            h_new[...] = h[part, cols(column * TF, TF)] + new

    @pl.when(step == pl.num_programs(0) - 1)
    def _():
        save.wait()
        for k in PLANE:

            @pl.loop(start_at, NT)
            def _(t, k=k):
                wait_bytes(totals("gu", t, k), ssem.at[k, t])

            if forward:

                @pl.loop(0, EARLY)
                def _(t, k=k):
                    wait_bytes(totals("next", t, k), ssem.at[k, CH + t])

        for kind, t, ch, due in late:
            for k in range(STAGES):
                if due[k] is not None:
                    wait_bytes(totals(kind, t, k), ssem.at[k, ch])


def gathered(h, shards, downs, other, number):
    forward = number == 0
    lead = LEAD if forward else LEAD_NEXT
    vmem, hbm = pl.BlockSpec(memory_space=pltpu.VMEM), pl.BlockSpec(memory_space=pl.ANY)
    tile = pl.BlockSpec((TOKENS, TF), lambda step: (0, upto(above(step - lead), NT - 1)))
    column = pl.BlockSpec((HALF, TF), lambda step: (above(step - lead - NT) % 2, above(step - lead - NT) // 2))
    row = pl.BlockSpec((TF, D), lambda step: (upto(above(step - lead), NT - 1), 0))
    shape, sems = jax.ShapeDtypeStruct, pltpu.SemaphoreType.DMA
    states, matrices = shape((TOKENS, D), BF), shape((NT, 2, NY, NZ, 2, RD, TF), BF)
    wide = [shape((TOKENS, FF), F32)] * 2
    return pl.pallas_call(
        functools.partial(gather_kernel, forward),
        grid=(lead + NT + (2 * ND if forward else 0),),
        in_specs=[vmem, vmem, vmem, *([] if forward else [vmem, hbm])],
        out_specs=[hbm, hbm, hbm, *([tile, tile, tile, column, hbm] if forward else [tile, tile, row])],
        out_shape=[
            matrices,
            shape((NY, NZ, 2, RF, D), BF),
            states,
            *([shape((TOKENS, FF), BF), *wide, states, matrices] if forward else [*wide, shape((FF, D), BF)]),
        ],
        scratch_shapes=[
            pltpu.VMEM((2, 2, NY, NZ, 2, RD, TF), BF),
            *([pltpu.VMEM((2, NY, NZ, 2, RF, TF), BF), pltpu.VMEM((TOKENS, FF), BF)] if forward else [pltpu.VMEM((TOKENS, TF), BF)]),
            pltpu.VMEM((TOKENS, D), BF),
            sems((STAGES, CH + EARLY)),
            sems((STAGES, CH + EARLY)),
            sems((2, 2)),
            sems((5,)),
        ],
        input_output_aliases={} if forward else {4: 0},
        compiler_params=pltpu.CompilerParams(
            collective_id=number, has_side_effects=True, vmem_limit_bytes=VMEM_LIMIT, dimension_semantics=("arbitrary",)
        ),
        name=f"gather_{number}",
    )(h, shards, downs, *other)


DC = LANES
STRIDE = {"gu": 1, "d": 2}
BIG, SMALL = {"gu": 4, "d": 2}, 2
NR = 8
NDC = D // DC


class Summing:
    HEIGHTS = {"gu": ((RD, RD), (RD, RD)), "d": ((40, 40), (40, RF - 120))}

    def __init__(self, kind, count, me, own, inbox, s1, r2, s2, r3, acc, s4, r4, s5, r5, xb, ssem, rsem, out):
        self.kind, self.count, self.me = kind, count, me
        self.stride, self.big = STRIDE[kind], BIG[kind]
        self.own, self.inbox, self.s1, self.r2, self.s2, self.r3 = own, inbox, s1, r2, s2, r3
        self.acc, self.s4, self.r4, self.s5, self.r5, self.xb = acc, s4, r4, s5, r5, xb
        self.ssem, self.rsem, self.out = ssem, rsem, out
        self.subs = (slice(None),) if kind == "gu" else (0, 1)

    def due(self, i, k):
        passed = i - 1 - k
        t = lax.div(passed, self.stride)
        return t, (passed >= 0) & (t < self.count) & (lax.rem(passed, self.stride) == 0)

    def part(self, half, sub):
        if self.kind == "gu":
            return sub, slice(None), pl.ds(half * LANES, LANES)
        low = 80 * half + 40 * sub
        return 0, pl.ds(low, self.HEIGHTS["d"][half][sub]), slice(None)

    def rows(self, half, sub):
        return slice(None) if self.kind == "gu" else pl.ds(0, self.HEIGHTS["d"][half][sub])

    def both(self, slot, y, z, half, sub):
        lead, rows, columns = self.part(half, sub)
        mine = self.own[slot, lead, y, z, self.me.c, rows, columns] if self.kind == "gu" else self.own[slot, y, z, rows, columns]
        theirs = self.inbox[slot, lead, y, z, rows, columns] if self.kind == "gu" else self.inbox[slot, y, z, rows, columns]
        return mine.astype(F32) + theirs.astype(F32)

    def size(self, k, slot, two):
        if k == 0:
            return self.inbox.at[slot]
        if k == 5:
            return self.xb.at[two, pl.ds(0, 3)]
        if self.kind == "gu":
            return (self.r2, self.r3, self.r4, self.r5)[k - 1].at[two]
        return self.inbox.at[(slot, *((0,), (pl.ds(0, 2),), (0, 0), (0, pl.ds(0, 2)))[k - 1])]

    def compute(self, k, t):
        me, slot, two = self.me, lax.rem(t, self.big), lax.rem(t, SMALL)
        if k > 0:
            wait_bytes(self.size(k - 1, slot, two), self.rsem.at[k - 1, slot])
            wait_bytes(self.size(k - 1, slot, two), self.ssem.at[k - 1, slot])
        if k == 6:
            total = self.xb[two, 0].astype(F32)
            for x in range(1, NX):
                total = total + self.xb[two, x].astype(F32)
            if self.kind == "gu":
                self.out[:, :, cols(t * TF, TF)] = total.astype(BF)
            else:
                self.out[:, cols(t * DC, DC)] = total.astype(BF)
            return
        for half in (0, 1):
            first, second = AXES[half]
            along = lambda place: (place, slice(None)) if first == 0 else (slice(None), place)
            for sub in (0, 1):
                rows = self.rows(half, sub)
                if k == 1:
                    self.s1[half, sub, :, rows] = self.both(slot, *along(me.ring(first, 2)), half, sub).astype(BF)
                if k == 2:
                    for way, by in WAYS:
                        term = self.both(slot, *along(me.ring(first, by)), half, sub)
                        if sub == way:
                            term = term + self.r2[two, half, sub, :, rows].astype(F32)
                        self.s2[half, way, sub, :, rows] = term.astype(BF)
                if k == 3:
                    term = self.both(slot, *along(me.pos[first]), half, sub)
                    for way in (0, 1):
                        term = term + self.r3[two, half, way, sub, :, rows].astype(F32)
                    self.acc[two, half, sub, :, rows] = term
                    self.s4[half, sub, rows] = self.acc[two, half, sub, me.ring(second, 2), rows].astype(BF)
                if k == 4:
                    for way, by in WAYS:
                        term = self.acc[two, half, sub, me.ring(second, by), rows]
                        if sub == way:
                            term = term + self.r4[two, half, sub, rows].astype(F32)
                        self.s5[half, way, sub, rows] = term.astype(BF)
                if k == 5:
                    term = self.acc[two, half, sub, me.pos[second], rows]
                    for way in (0, 1):
                        term = term + self.r5[two, half, way, sub, rows].astype(F32)
                    lead, where, columns = self.part(half, sub)
                    if self.kind == "gu":
                        self.xb[two, me.x, lead, where, columns] = term.astype(BF)
                    else:
                        self.xb[two, me.x, where, columns] = term.astype(BF)

    def send(self, k, t, source=None):
        me, slot, two = self.me, lax.rem(t, self.big), lax.rem(t, SMALL)

        def go(src, dst, peer):
            pltpu.make_async_remote_copy(
                src_ref=src, dst_ref=dst, send_sem=self.ssem.at[k, slot], recv_sem=self.rsem.at[k, slot], device_id=peer, device_id_type=MESH
            ).start()

        if k == 0:
            go(source, self.inbox.at[slot], me.partner())
        if k == 5:
            for by in OTHERS:
                go(self.xb.at[two, me.x], self.xb.at[two, me.x], me.across(by))
        for half in (0, 1):
            first, second = AXES[half]
            for way, by in WAYS:
                if k == 1:
                    rows = self.rows(half, way)
                    go(self.s1.at[half, way, :, rows], self.r2.at[two, half, way, :, rows], me.near(first, by))
                if k == 3:
                    rows = self.rows(half, way)
                    go(self.s4.at[half, way, rows], self.r4.at[two, half, way, rows], me.near(second, by))
                if k in (2, 4):
                    for sub in self.subs:
                        rows = self.rows(half, sub)
                        if k == 2:
                            go(self.s2.at[half, way, sub, :, rows], self.r3.at[two, half, way, sub, :, rows], me.near(first, by))
                        else:
                            go(self.s5.at[half, way, sub, rows], self.r5.at[two, half, way, sub, rows], me.near(second, by))


def stage_buffers(kind):
    block, last = ((2, NY, NZ, RD, TF), (2, RD, TF)) if kind == "gu" else ((NY, NZ, RF, DC), (RF, DC))
    big, piece, halves = BIG[kind], (40, LANES), (2, 2)
    many = (4, *piece)
    vmem, sems = lambda *dims: pltpu.VMEM(dims, BF), pltpu.SemaphoreType.DMA
    return [
        vmem(big, 2, NY, NZ, 2, RD, TF) if kind == "gu" else vmem(big, *block),
        vmem(big, *block),
        vmem(*halves, *many),
        vmem(SMALL, *halves, *many),
        vmem(2, *halves, *many),
        vmem(SMALL, 2, *halves, *many),
        pltpu.VMEM((SMALL, *halves, *many), F32),
        vmem(*halves, *piece),
        vmem(SMALL, *halves, *piece),
        vmem(2, *halves, *piece),
        vmem(SMALL, 2, *halves, *piece),
        vmem(SMALL, NX, *last),
        sems((6, big)),
        sems((6, big)),
    ]


NBUF = 14


def sum_over_group(me, value, out, bufs, ssem, rsem):
    rings = [[me.near(axis, by) for by in OTHERS] for axis in (0, 1)] + [[me.partner()]]
    for k, (buf, place, ring) in enumerate(zip(bufs, (me.y, me.z, me.c), rings)):
        buf[place] = value
        for peer in ring:
            pltpu.make_async_remote_copy(
                src_ref=buf.at[place], dst_ref=buf.at[place], send_sem=ssem.at[k], recv_sem=rsem.at[k], device_id=peer, device_id_type=MESH
            ).start()
        wait_bytes(buf.at[pl.ds(0, len(ring))], rsem.at[k])
        wait_bytes(buf.at[pl.ds(0, len(ring))], ssem.at[k])
        value = buf[0]
        for n in range(1, len(ring) + 1):
            value = value + buf[n]
    out[...] = value


def back_kernel(with_da, *refs):
    refs = list(refs)
    take = lambda n: [refs.pop(0) for _ in range(n)]
    a, dy_in, wd, gate, up, dwd = take(6)
    if with_da:
        wgu, h, act = take(3)
        out_gu, out_d, dh, dwd_next = take(4)
    else:
        parts = take(2)
        out_gu, out_d, total = take(3)
    gu_bufs, d_bufs = take(NBUF), take(NBUF)
    dg_s, du_s, lsem = take(3)
    dy = dy_in
    if with_da:
        da, dy, dsem = take(3)
    else:
        rings = take(3)
        tsems = take(2)
    i = pl.program_id(0)
    me = Place()
    bring = pltpu.make_async_copy(dy_in, dy, dsem.at[0]) if with_da else None
    save = pltpu.make_async_copy(dy, dh, dsem.at[1]) if with_da else None

    @pl.when(i == 0)
    def _():
        if with_da:
            bring.start()
        me.meet(True, not with_da)
        if with_da:
            bring.wait()

    own = gu_bufs[0]
    gu = Summing("gu", NT, me, *gu_bufs, out_gu)
    down = Summing("d", NDC, me, *d_bufs, out_d)

    def load(n):
        slot = lax.rem(n, down.big)
        return pltpu.make_async_copy(dwd.at[:, :, me.c, :, cols(n * DC, DC)], down.own.at[slot], lsem.at[slot])

    for k in range(6, 0, -1):
        for engine in (gu, down):
            t, there = engine.due(i, k)

            @pl.when(there)
            def _(k=k, engine=engine, t=t):
                if k == 1 and engine is down:
                    load(t).wait()
                engine.compute(k, t)

    for k in reversed(range(6)):
        for engine in (gu, down):
            t, there = engine.due(i, k)

            @pl.when(there)
            def _(k=k, engine=engine, t=t):
                source = None
                if k == 0:
                    source = own.at[lax.rem(t, gu.big), :, :, :, 1 - me.c] if engine is gu else dwd.at[:, :, 1 - me.c, :, cols(t * DC, DC)]
                engine.send(k, t, source)

    @pl.when((i < NDC * down.stride) & (lax.rem(i, down.stride) == 0))
    def _():
        load(lax.div(i, down.stride)).start()

    @pl.when(i < NT)
    def _():
        slot = lax.rem(i, gu.big)
        rows = TOKENS // 4
        for r in range(4):
            part = pl.ds(r * rows, rows)
            dh = dot(dy[part, :], wd[...], 1, 1).astype(BF).astype(F32)
            g, u = gate[part, :], up[part, :]
            sg = jax.nn.sigmoid(g)
            du_s[part, :] = (dh * (g * sg)).astype(BF)
            dg_s[part, :] = (dh * u * (sg * (1 + g * (1 - sg)))).astype(BF)
        own[slot, 0] = dot(a[...], dg_s[...], 0, 0).reshape(NY, NZ, 2, RD, TF).astype(BF)
        own[slot, 1] = dot(a[...], du_s[...], 0, 0).reshape(NY, NZ, 2, RD, TF).astype(BF)
        if with_da:
            more = dot(dg_s[...], wgu[0], 1, 1) + dot(du_s[...], wgu[1], 1, 1)

            @pl.when(i == 0)
            def _():
                da[...] = more

            @pl.when(i > 0)
            def _():
                da[...] += more

    if not with_da:

        @pl.when(i == pl.num_programs(0) - 1)
        def _():
            squares = jnp.zeros((8, 128), F32)
            for ref in (*parts, out_gu, out_d):
                for block in (ref,) if len(ref.shape) == 2 else (ref.at[0], ref.at[1]):
                    squares = squares + jnp.sum(block[...].astype(F32) ** 2)
            sum_over_group(me, squares, total, rings, *tsems)

        return

    @pl.when((i >= NT) & (i < NT + NR))
    def _():
        rows = TOKENS // NR
        part = pl.ds(pl.multiple_of((i - NT) * rows, rows), rows)
        wide, by_a = h[...].astype(F32), da[part, :].astype(BF).astype(F32)
        scale = lax.rsqrt(jnp.mean(wide**2, -1, keepdims=True) + 1e-6)
        by_h = by_a * scale - wide * (scale * scale * scale * jnp.mean(by_a * wide, -1, keepdims=True))
        dy[part, :] = dy[part, :] + by_h.astype(BF)

    @pl.when(i == NT + NR)
    def _():
        save.start()

    tiles = (dg_s, du_s)

    def bring_act(t, slot):
        return pltpu.make_async_copy(act.at[:, cols(t * TF, TF)], tiles[slot], dsem.at[2 + slot])

    @pl.when(i == NT + NR - 1)
    def _():
        bring_act(0, 0).start()

    t = i - NT - NR
    for slot in (0, 1):

        @pl.when((t >= 0) & (lax.rem(t, 2) == slot))
        def _(slot=slot):
            bring_act(t, slot).wait()

            @pl.when(t < NT - 1)
            def _():
                bring_act(t + 1, 1 - slot).start()

            dwd_next[...] = dot(tiles[slot][...], dy[...], 0, 0).astype(BF)

    @pl.when(i == pl.num_programs(0) - 1)
    def _():
        save.wait()


def backward(a, dy, g_d, gate, up, dwd, more, number):
    with_da = number == 2
    vmem, hbm = pl.BlockSpec(memory_space=pltpu.VMEM), pl.BlockSpec(memory_space=pl.ANY)
    shape, sems = jax.ShapeDtypeStruct, pltpu.SemaphoreType.DMA
    tile = pl.BlockSpec((TOKENS, TF), lambda i: (0, upto(i, NT - 1)))
    in_specs = [vmem, hbm if with_da else vmem, pl.BlockSpec((TF, D), lambda i: (upto(i, NT - 1), 0)), tile, tile, hbm]
    out_specs, out_shape = [vmem, vmem], [shape((2, RD, FF), BF), shape((RF, D), BF)]
    scratch = []
    if with_da:
        late = lambda i: above(i - NT - NR)
        in_specs += [
            pl.BlockSpec((None, 2, D, TF), lambda i: (upto(i, NT - 1), 0, 0, 0)),
            pl.BlockSpec((TOKENS // NR, D), lambda i: (upto(above(i - NT), NR - 1), 0)),
            hbm,
        ]
        out_specs += [hbm, pl.BlockSpec((TF, D), lambda i: (late(i), 0))]
        out_shape += [shape((TOKENS, D), BF), shape((FF, D), BF)]
        scratch = [pltpu.VMEM((TOKENS, D), F32), pltpu.VMEM((TOKENS, D), BF), sems((4,))]
    else:
        tiny = (8, 128)
        in_specs += [vmem, vmem]
        out_specs += [vmem]
        out_shape += [shape(tiny, F32)]
        scratch = [*(pltpu.VMEM((n, *tiny), F32) for n in (NY, NZ, 2)), sems((3,)), sems((3,))]
    return pl.pallas_call(
        functools.partial(back_kernel, with_da),
        grid=(2 * NT + NR if with_da else NT + STAGES,),
        in_specs=in_specs,
        out_specs=out_specs,
        out_shape=out_shape,
        scratch_shapes=[
            *stage_buffers("gu"),
            *stage_buffers("d"),
            pltpu.VMEM((TOKENS, TF), BF),
            pltpu.VMEM((TOKENS, TF), BF),
            sems((BIG["d"],)),
            *scratch,
        ],
        compiler_params=pltpu.CompilerParams(
            collective_id=number, has_side_effects=True, vmem_limit_bytes=VMEM_LIMIT, dimension_semantics=("arbitrary",)
        ),
        name=f"backward_{number}",
    )(a, dy, g_d, gate, up, dwd.reshape(NY, NZ, 2, RF, D), *more)


def normed(h):
    wide = h.astype(F32)
    scale = lax.rsqrt(jnp.mean(wide**2, -1, keepdims=True) + 1e-6)
    return (wide * scale).astype(BF)


def adamw(w, m, v, g):
    m = 0.9 * m + 0.1 * g
    v = 0.95 * v + 0.05 * g * g
    step = m * lax.rsqrt(v + 1e-8) + 0.1 * w
    return (w - 0.02 * step).astype(BF), m, v


def clipped(gradients, sum_of_squares, count):
    factor = jnp.minimum(1.0, 0.5 * lax.rsqrt(sum_of_squares / count + 1e-30))
    return [g * factor for g in gradients]


def solution(mesh):
    def step(x, dy, *arrays):
        weights, m, v = (arrays[i : i + 3] for i in (0, 3, 6))
        shards = jnp.stack(weights[:2], 1), weights[2]
        h0, dy = x[0], dy[0]
        _, d0, a0, act0, gate0, up0, h1, first = gathered(h0, *shards, [], 0)
        gu1, d1, a1, gate1, up1, by_d1 = gathered(h1, *shards, [dy, first], 1)
        gu1, d0, d1 = gu1.reshape(NT, 2, D, TF), d0.reshape(FF, D), d1.reshape(FF, D)
        mine_gu1, mine_d1, dh, by_d0 = backward(a1, dy, d1, gate1, up1, by_d1, (gu1, h1, act0), 2)
        mine_gu0, mine_d0, squares = backward(a0, dh, d0, gate0, up0, by_d0, (mine_gu1, mine_d1), 3)
        gradients = [jnp.stack([mine_gu0[n], mine_gu1[n]]).astype(F32) for n in (0, 1)] + [jnp.stack([mine_d0, mine_d1]).astype(F32)]
        gradients = clipped(gradients, squares[0, 0], S * sum(g.size for g in gradients))
        new = [adamw(w.astype(F32), m, v, g) for w, m, v, g in zip(weights, m, v, gradients, strict=True)]
        return tuple(one[which] for which in range(3) for one in new)

    states, cut = P(("rep", "r", "s"), None, None), P(None, "s", None)
    return jax.shard_map(
        step,
        mesh=mesh,
        in_specs=(states, states) + (cut,) * 9,
        out_specs=(P("rep", "s", None),) * 9,
        check_vma=False,
    )
```
